128 devices in a mesh: ctx: 16 (over x, y), head: 8 (over z, core).
Axes of the slice: x: 4, y: 4, z: 4, core: 2. Of those that a mesh axis runs over, the one named last changes fastest.
Arguments:
- query_low: bfloat16 [2, 1536], P(None, 'ctx'), may hold values from -6 to 6
- query_weight: bfloat16 [1536, 73728], P('ctx', 'head'), may hold values from -0.21875 to 0.21875
- latent_cache: bfloat16 [2, 131072, 576], P(None, ('ctx', 'head')), may hold values from -300 to 300
- lengths: int32 [2], replicated, may hold values from 81921 to 131072
- value_weight: bfloat16 [128, 512, 128], P('head'), may hold values from -2 to 2
- output_weight: bfloat16 [16384, 7168], P('head', 'ctx'), may hold values from -0.0625 to 0.0625
Outputs:
- attended: bfloat16 [2, 7168], P(None, ('ctx', 'head'))
The draws below stay inside these ranges and needn't reach their ends.
All inputs are finite; a program needn't handle non-finite values.
Results may differ from the reference program's by a relative error of at most 0.028.
Values may be sent and summed in bfloat16 or wider, within the bound.
No kernel may reach another device: no remote copies, remote signals or barrier semaphores. Data moves between devices by JAX's collectives and lax.ppermute only.
A program may use at most 192 MiB of HBM per device.

```python
import jax
import jax.numpy as jnp
from jax import lax

D = 7168
HEADS = 128
QL = 1536
KV_RANK = 512
ROPE_DIM = 64
V_DIM = 128
SEQS = 2
CTX_DEV = 1024
LENGTH = 131072


def draw_latent_cache(key, part):
    width = KV_RANK + ROPE_DIM

    def one_sequence(sequence):
        row_key = jax.random.fold_in(key, sequence)
        common = jnp.clip(jax.random.normal(jax.random.fold_in(row_key, 11), (KV_RANK,), jnp.float32), -3.0, 3.0)
        fraction = jnp.arange(LENGTH, dtype=jnp.float32) / LENGTH
        values = jnp.clip(jax.random.normal(row_key, (LENGTH, width), jnp.float32), -6.0, 6.0)
        ramp = 3.0 * fraction - 1.0
        latent = values[:, :KV_RANK] + ramp[:, None] * common[None, :]
        values = jnp.concatenate([latent, values[:, KV_RANK:]], axis=1)
        return values.astype(jnp.bfloat16)
    return lax.map(one_sequence, jnp.arange(SEQS))


def spiked(array, stream_key, source, target, blocks, factor):
    def block_of(dim):
        return (jnp.arange(array.shape[dim]) // (array.shape[dim] // blocks)).reshape((-1,) + (1,) * (array.ndim - 1 - dim))

    one_side = jax.random.permutation(stream_key, blocks)[block_of(target)]
    second = (block_of(target) + blocks // 2) % blocks
    return jnp.where((block_of(source) == one_side) | (block_of(source) == second), factor * array, array)


def block_scale(key, extent, split, low, largest):
    gain, own = 1.0, jax.random.fold_in(key, 6)
    for axis_at, blocks in split:
        steps = jnp.exp(jax.random.uniform(jax.random.fold_in(own, axis_at), (blocks,), jnp.float32, low / len(split), largest / len(split)))
        gain = gain * jnp.repeat(steps, extent[axis_at] // blocks).reshape([-1 if axis == axis_at else 1 for axis in range(len(extent))])
    return gain


def normal_values(stream_key, extent, deviation, reach, shards=(), kind=jnp.bfloat16):
    factor_of = block_scale(stream_key, extent, shards, -0.22, 0.18) if shards else 1.0
    result = jax.random.normal(stream_key, extent, jnp.float32) * deviation * factor_of
    return jnp.minimum(jnp.maximum(result, -reach), reach).astype(kind)


def noise_with(own_key, shape, deviation, limit, shards, heavy, kind=jnp.bfloat16):
    drawn = deviation * jax.random.normal(own_key, shape, jnp.float32)
    if shards:
        drawn = drawn * block_scale(own_key, shape, shards, -0.22, 0.18)
    return jnp.clip(spiked(drawn, jax.random.fold_in(own_key, 3), *heavy), -limit, limit).astype(kind)


def setup_inputs(seed: int = 0) -> dict:
    seeds = jax.random.split(jax.random.key(seed), 7)
    query_low = normal_values(seeds[0], (SEQS, QL), 1.0, 6.0, ((1, 16),))
    query_weight = normal_values(seeds[1], (QL, HEADS * (KV_RANK + ROPE_DIM)), (QL // 2) ** -0.5, 0.21875, ((0, 16), (1, 8)))
    latent_cache = draw_latent_cache(jax.random.fold_in(seeds[6], 71), 0)
    lengths = jax.random.randint(seeds[3], (SEQS,), LENGTH * 5 // 8 + 1, LENGTH + 1).astype(jnp.int32)
    value_weight = normal_values(seeds[4], (HEADS, KV_RANK, V_DIM), (KV_RANK // 64) ** -0.5, 2.0, ((0, 8),))
    output_weight = noise_with(seeds[5], (HEADS * V_DIM, D), (HEADS * V_DIM) ** -0.5, 0.0625, ((0, 8), (1, 16)), (0, 1, 16, 2.0))
    return {"query_low": query_low, "query_weight": query_weight, "latent_cache": latent_cache, "lengths": lengths, "value_weight": value_weight, "output_weight": output_weight}


softmax_scale = 0.07216878


def reference(query_low, query_weight, latent_cache, lengths, value_weight, output_weight):
    sequences = query_low.shape[0]
    head_count = value_weight.shape[0]
    rounded = jnp.dot(query_low, query_weight, preferred_element_type=jnp.float32).astype(jnp.bfloat16)
    queries = lax.optimization_barrier(rounded).reshape(sequences, head_count, -1).astype(jnp.float32)
    block_count = LENGTH // CTX_DEV

    def advance(running, block_index):
        maximum, totals, numerators = running
        offset = (block_index * CTX_DEV).astype(jnp.int32)
        pieces = lax.dynamic_slice_in_dim(latent_cache, offset, CTX_DEV, 1).astype(jnp.float32)
        scores = jnp.einsum("bhc,bpc->bhp", queries, pieces) * softmax_scale
        places = offset + jnp.arange(CTX_DEV, dtype=jnp.int32)
        usable = (places[None, :] < lengths[:, None])[:, None, :]
        scores = jnp.where(usable, scores, -1e30)
        block_max = jnp.max(scores, axis=2)
        probabilities = jnp.where(usable, jnp.exp(scores - block_max[..., None]), 0.0)
        block_total = jnp.sum(probabilities, axis=2)
        weights = lax.optimization_barrier(probabilities.astype(jnp.bfloat16)).astype(jnp.float32)
        block_numerator = jnp.einsum("bhp,bpc->bhc", weights, pieces[:, :, :KV_RANK])
        highest = jnp.maximum(maximum, block_max)
        old_scale = jnp.exp(maximum - highest)
        new_scale = jnp.exp(block_max - highest)
        totals = totals * old_scale + block_total * new_scale
        numerators = numerators * old_scale[..., None] + block_numerator * new_scale[..., None]
        return (highest, totals, numerators), None

    start_state = (jnp.full((sequences, head_count), -1e30, jnp.float32),
                   jnp.zeros((sequences, head_count), jnp.float32),
                   jnp.zeros((sequences, head_count, KV_RANK), jnp.float32))
    final_state, _ = lax.scan(advance, start_state, jnp.arange(block_count, dtype=jnp.int32))
    latent_out = (final_state[2] / final_state[1][..., None]).astype(jnp.bfloat16)
    values = jnp.einsum("bhc,hcv->bhv", latent_out.astype(jnp.float32), value_weight.astype(jnp.float32)).astype(jnp.bfloat16)
    return jnp.dot(values.reshape(sequences, -1), output_weight, preferred_element_type=jnp.float32).astype(jnp.bfloat16)
```

```python
import jax
import jax.numpy as jnp
from jax import lax
from jax.sharding import Mesh
from jax.sharding import PartitionSpec as P

KV_RANK = 512
CTX = ("ctx_0", "ctx_1")
HEAD = ("head_0", "head_1")
CTX_HEAD = CTX + HEAD
HEAD_CTX = HEAD + CTX
SCALE = 0.07216878
LANES = 128


def exchange(x, axes):
    return lax.all_to_all(x, axes, 0, 0, tiled=True)


def to_all(x, axes):
    return exchange(jnp.broadcast_to(x, (lax.axis_size(axes), *x.shape)), axes)


def three_terms(x):
    high = lax.reduce_precision(x, 8, 7)
    rest = x - high
    middle = lax.reduce_precision(rest, 8, 7)
    low = rest - middle
    return [term.astype(jnp.bfloat16) for term in (high, middle, low)]


def packed(vectors, top, total):
    seqs, heads, _ = vectors.shape
    rows = jnp.swapaxes(vectors, 0, 1).reshape(heads, -1).astype(jnp.bfloat16)
    terms = jnp.concatenate(three_terms(top) + three_terms(total), axis=0).T
    terms = jnp.pad(terms, ((0, 0), (0, LANES - terms.shape[1])))
    return jnp.concatenate([rows, terms], axis=1)


def combined(parts, seqs):
    peers, heads, width = parts.shape
    terms = parts[:, :, width - LANES :].astype(jnp.float32)
    terms = terms[:, :, : 6 * seqs].reshape(peers, heads, 2, 3, seqs).sum(axis=3)
    tops, totals = terms[:, :, 0], terms[:, :, 1]
    top = jnp.max(tops, axis=0)
    factor = jnp.exp(tops - top)
    total = jnp.sum(totals * factor, axis=0)
    vectors = parts[:, :, : width - LANES].reshape(peers, heads, seqs, -1)
    summed = jnp.sum(vectors.astype(jnp.float32) * factor[..., None], axis=0)
    return summed, top, total


def on_device(query_low, query_weight, latent_cache, lengths, value_weight, output_weight):
    ctx_count = lax.axis_size(CTX)
    head_count = lax.axis_size(HEAD)
    seqs = query_low.shape[0]
    local_heads = value_weight.shape[0]
    width = latent_cache.shape[2]
    span = latent_cache.shape[1]

    partial = jnp.dot(query_low, query_weight, preferred_element_type=jnp.float32)
    partial = jnp.swapaxes(partial.reshape(seqs, ctx_count, -1), 0, 1)
    own = exchange(partial, CTX).sum(axis=0).astype(jnp.bfloat16)
    queries = to_all(own, HEAD_CTX).reshape(local_heads * head_count, seqs, width)

    offset = (lax.axis_index(CTX) * head_count + lax.axis_index(HEAD)) * span
    places = offset + jnp.arange(span, dtype=jnp.int32)
    usable = (places[None, :] < lengths[:, None])[:, None, :]
    scores = jnp.einsum(
        "hbc,bpc->bhp", queries, latent_cache, preferred_element_type=jnp.float32
    )
    scores = jnp.where(usable, scores * SCALE, -1e30)
    top = jnp.max(scores, axis=2)
    weights = jnp.where(usable, jnp.exp(scores - top[..., None]), 0.0)
    total = jnp.sum(weights, axis=2)
    numerators = jnp.einsum(
        "bhp,bpc->bhc",
        weights.astype(jnp.bfloat16),
        latent_cache[:, :, :KV_RANK],
        preferred_element_type=jnp.float32,
    )
    sent = packed(numerators, top, total).reshape(head_count, local_heads, -1)
    numerators, top, total = combined(exchange(sent, HEAD), seqs)
    values = jnp.einsum(
        "hbc,hcv->bhv",
        numerators.astype(jnp.bfloat16),
        value_weight,
        preferred_element_type=jnp.float32,
    )
    values, _, total = combined(to_all(packed(values, top.T, total.T), CTX), seqs)
    values = (values / total[..., None]).astype(jnp.bfloat16)
    values = jnp.swapaxes(values, 0, 1).reshape(seqs, -1)
    projected = jnp.dot(values, output_weight, preferred_element_type=jnp.float32)
    projected = jnp.swapaxes(projected.reshape(seqs, head_count, -1), 0, 1)
    return exchange(projected, HEAD).sum(axis=0).astype(jnp.bfloat16)


def solution(mesh):
    finer = Mesh(mesh.devices.reshape(4, 4, 4, 2), CTX_HEAD)
    return jax.shard_map(
        on_device,
        mesh=finer,
        in_specs=(
            P(None, CTX),
            P(CTX, HEAD),
            P(None, CTX_HEAD, None),
            P(),
            P(HEAD, None, None),
            P(HEAD, CTX),
        ),
        out_specs=P(None, CTX_HEAD),
        check_vma=False,
    )
```

```python
import functools

import jax
import jax.numpy as jnp
from jax import lax
from jax.experimental import pallas as pl
from jax.experimental.pallas import tpu as pltpu
from jax.sharding import Mesh
from jax.sharding import PartitionSpec as P

KV_RANK = 512
CTX = ("ctx_0", "ctx_1")
HEAD = ("head_0", "head_1")
CTX_HEAD = CTX + HEAD
GATHER = ("head_0", "ctx_0")
SCALE = 0.07216878
MASKED = -1e30
FLOOR = -1e29
LANES = 128
LAST = (((1,), (1,)), ((), ()))
F32 = jnp.float32
BF16 = jnp.bfloat16

VMEM = pl.BlockSpec(memory_space=pltpu.VMEM)
SMEM = pl.BlockSpec(memory_space=pltpu.SMEM)
HBM = pl.BlockSpec(memory_space=pltpu.HBM)


def exchange(x, axes):
    return lax.all_to_all(x, axes, 0, 0, tiled=True)


def three_terms(x):
    high = x.astype(BF16).astype(F32)
    rest = x - high
    middle = rest.astype(BF16).astype(F32)
    return high, middle, rest - middle


def terms_tile(top, total):
    rows, seqs = top.shape
    lane = lax.broadcasted_iota(jnp.int32, (rows, LANES), 1)
    tile = jnp.zeros((rows, LANES), F32)
    at = 0
    for part in three_terms(top) + three_terms(total):
        for b in range(seqs):
            tile = jnp.where(lane == at, part[:, b : b + 1], tile)
            at += 1
    return tile.astype(BF16)


def from_terms(tile, seqs):
    tile = tile.astype(F32)
    part = [tile[:, k * seqs : (k + 1) * seqs] for k in range(6)]
    return part[0] + part[1] + part[2], part[3] + part[4] + part[5]


def rescaled(tiles, seqs):
    pairs = [from_terms(tile, seqs) for tile in tiles]
    top = functools.reduce(jnp.maximum, [t for t, _ in pairs])
    factors = [jnp.exp(t - top) for t, _ in pairs]
    total = sum(n * f for (_, n), f in zip(pairs, factors))
    return top, total, factors


def project_queries(chunks, copies, low_ref, weight_ref, out_ref, held, sems):
    width = held.shape[2]
    loads = [
        pltpu.make_async_copy(
            weight_ref.at[:, pl.ds(k * width, width)], held.at[k], sems.at[k]
        )
        for k in range(chunks)
    ]
    for load in loads:
        load.start()
    low = low_ref[...]
    for k in range(chunks):
        loads[k].wait()
        part = jnp.dot(low, held[k], preferred_element_type=F32)
        for n in range(copies):
            out_ref[k * copies + n] = part


def sum_queries(parts_ref, out_ref, rows):
    peers, seqs, _ = parts_ref.shape
    width = out_ref.shape[2]
    heads = out_ref.shape[1] // seqs
    total = parts_ref[0]
    for k in range(1, peers):
        total = total + parts_ref[k]
    for b in range(seqs):
        for j in range(heads):
            rows[b * heads + j : b * heads + j + 1, :] = total[
                b : b + 1, j * width : (j + 1) * width
            ]
    done = rows[...].astype(BF16)
    for k in range(out_ref.shape[0]):
        out_ref[k] = done


def attend(lengths_ref, query_ref, own_ref, other_ref, out_ref, rows):
    groups, both, width = query_ref.shape
    seqs, _, span = own_ref.shape
    each = both // seqs
    heads = groups * each
    core = lax.axis_index("head_1")
    pair = (
        lax.axis_index(CTX) * lax.axis_size("head_0") + lax.axis_index("head_0")
    ) * lax.axis_size("head_1")
    starts = ((pair + core) * span, (pair + 1 - core) * span)
    for g in range(groups):
        for b in range(seqs):
            rows[b, g * each : (g + 1) * each, :] = query_ref[
                g, b * each : (b + 1) * each, :
            ].astype(F32)
    tops, totals = [], []
    place = lax.broadcasted_iota(jnp.int32, (heads, span), 1)
    share = out_ref.shape[1]
    for b in range(seqs):
        query = rows[b].astype(BF16)
        scores = []
        for start, block in zip(starts, (own_ref, other_ref)):
            raw = jnp.dot(query, block[b], preferred_element_type=F32)
            scores.append(jnp.where(place < lengths_ref[b] - start, raw * SCALE, MASKED))
        top = jnp.maximum(
            jnp.max(scores[0], axis=1, keepdims=True),
            jnp.max(scores[1], axis=1, keepdims=True),
        )
        top = jnp.maximum(top, FLOOR)
        weights = [jnp.exp(s - top) for s in scores]
        total = jnp.sum(weights[0], axis=1, keepdims=True) + jnp.sum(
            weights[1], axis=1, keepdims=True
        )
        numerator = sum(
            lax.dot_general(w.astype(BF16), block[b, :KV_RANK, :], LAST, preferred_element_type=F32)
            for w, block in zip(weights, (own_ref, other_ref))
        ).astype(BF16)
        for k in range(out_ref.shape[0]):
            out_ref[k, :, b * KV_RANK : (b + 1) * KV_RANK] = numerator[
                k * share : (k + 1) * share
            ]
        tops.append(top)
        totals.append(total)
    lane = lax.broadcasted_iota(jnp.int32, (heads, LANES), 1)
    top = jnp.where(lane == 0, tops[0], tops[1])[:, :seqs]
    total = jnp.where(lane == 0, totals[0], totals[1])[:, :seqs]
    tile = terms_tile(top, total)
    for k in range(out_ref.shape[0]):
        out_ref[k, :, seqs * KV_RANK :] = tile[k * share : (k + 1) * share]


def project_values(parts_ref, weight_ref, out_ref):
    peers, heads, width = parts_ref.shape
    seqs = (width - LANES) // KV_RANK
    top, total, factors = rescaled(
        [parts_ref[k, :, width - LANES :] for k in range(peers)], seqs
    )
    halves = []
    for b in range(seqs):
        halves.append(
            sum(
                parts_ref[k, :, b * KV_RANK : (b + 1) * KV_RANK].astype(F32)
                * factors[k][:, b : b + 1]
                for k in range(peers)
            )
        )
    stacked = jnp.concatenate(halves, axis=0).astype(BF16)
    row = lax.broadcasted_iota(jnp.int32, (seqs * heads, LANES), 0)
    values = jnp.zeros((seqs * heads, LANES), F32)
    for h in range(heads):
        one = jnp.dot(stacked, weight_ref[h], preferred_element_type=F32)
        values = jnp.where(lax.rem(row, heads) == h, one, values)
    values = values.astype(BF16)
    tile = terms_tile(top, total)
    for k in range(out_ref.shape[0]):
        out_ref[k, : seqs * heads, :] = values
        out_ref[k, seqs * heads :, :] = tile


def project_output(parts_ref, weight_ref, out_ref, flat):
    peers, rows, lanes = parts_ref.shape
    seqs = out_ref.shape[1]
    heads = rows // (seqs + 1)
    _, total, factors = rescaled(
        [parts_ref[k, seqs * heads :, :] for k in range(peers)], seqs
    )
    for b in range(seqs):
        values = sum(
            parts_ref[k, b * heads : (b + 1) * heads, :].astype(F32) * factors[k][:, b : b + 1]
            for k in range(peers)
        )
        values = values / total[:, b : b + 1]
        for h in range(heads):
            flat[b : b + 1, h * lanes : (h + 1) * lanes] = values[h : h + 1]
    result = lax.dot_general(
        flat[...].astype(BF16), weight_ref[...], LAST, preferred_element_type=F32
    )
    width = out_ref.shape[2]
    for k in range(out_ref.shape[0]):
        out_ref[k] = result[:, k * width : (k + 1) * width]


def call(body, name, out_shape, out_dtype, in_specs, scratch=(), limit=8):
    return pl.pallas_call(
        body,
        name=name,
        out_shape=jax.ShapeDtypeStruct(out_shape, out_dtype),
        in_specs=in_specs,
        out_specs=VMEM,
        scratch_shapes=list(scratch),
        compiler_params=pltpu.CompilerParams(vmem_limit_bytes=limit * 2**20),
    )


def on_device(query_low, query_weight, latent_cache, lengths, value_weight, output_weight):
    ctx_count = lax.axis_size(CTX)
    head_count = lax.axis_size(HEAD)
    chunks = lax.axis_size("ctx_0")
    depth_count = lax.axis_size("head_0")
    seqs, depth = query_low.shape
    local_heads = value_weight.shape[0]
    width = latent_cache.shape[2]
    columns = query_weight.shape[1]
    each = local_heads // chunks

    latent_cache = jnp.swapaxes(latent_cache, 1, 2)
    other_cache = lax.ppermute(latent_cache, "head_1", [(0, 1), (1, 0)])

    partial = call(
        functools.partial(project_queries, chunks, ctx_count // chunks),
        "project_queries",
        (ctx_count, seqs, columns // chunks),
        F32,
        [VMEM, HBM],
        [
            pltpu.VMEM((chunks, depth, columns // chunks), BF16),
            pltpu.SemaphoreType.DMA((chunks,)),
        ],
    )(query_low, query_weight)
    partial = exchange(partial, CTX)

    own = call(
        sum_queries,
        "sum_queries",
        (depth_count * chunks, seqs * each, width),
        BF16,
        [VMEM],
        [pltpu.VMEM((seqs * each, width), F32)],
    )(partial)
    queries = exchange(own, GATHER)

    sent = call(
        attend,
        "attend",
        (depth_count, local_heads, seqs * KV_RANK + LANES),
        BF16,
        [SMEM, VMEM, VMEM, VMEM],
        [pltpu.VMEM((seqs, depth_count * local_heads, width), F32)],
        limit=24,
    )(lengths, queries, latent_cache, other_cache)
    arrived = exchange(sent, "head_0")

    values = call(
        project_values,
        "project_values",
        (ctx_count, (seqs + 1) * local_heads, value_weight.shape[2]),
        BF16,
        [VMEM, VMEM],
    )(arrived, value_weight)
    values = exchange(values, CTX)

    projected = call(
        project_output,
        "project_output",
        (head_count, seqs, output_weight.shape[1] // head_count),
        F32,
        [VMEM, VMEM],
        [pltpu.VMEM((seqs, output_weight.shape[0]), F32)],
    )(values, output_weight.T)
    return exchange(projected, HEAD).sum(axis=0).astype(BF16)


def solution(mesh):
    finer = Mesh(mesh.devices.reshape(4, 4, 4, 2), CTX_HEAD)
    return jax.shard_map(
        on_device,
        mesh=finer,
        in_specs=(
            P(None, CTX),
            P(CTX, HEAD),
            P(None, CTX_HEAD, None),
            P(),
            P(HEAD, None, None),
            P(HEAD, CTX),
        ),
        out_specs=P(None, CTX_HEAD),
        check_vma=False,
    )
```

```python
import functools

import jax
import jax.numpy as jnp
from jax import lax
from jax.experimental import pallas as pl
from jax.experimental.pallas import tpu as pltpu
from jax.sharding import Mesh
from jax.sharding import PartitionSpec as P

KV_RANK = 512
CTX = ("ctx_0", "ctx_1")
HEAD = ("head_0", "head_1")
CTX_HEAD = CTX + HEAD
GATHER = ("head_0", "ctx_0")
SCALE = 0.07216878
MASKED = -1e30
FLOOR = -1e29
LANES = 128
LAST = (((1,), (1,)), ((), ()))
F32 = jnp.float32
BF16 = jnp.bfloat16

VMEM = pl.BlockSpec(memory_space=pltpu.VMEM)
HBM = pl.BlockSpec(memory_space=pltpu.HBM)


def exchange(x, axes):
    return lax.all_to_all(x, axes, 0, 0, tiled=True)


def three_terms(x):
    high = x.astype(BF16).astype(F32)
    rest = x - high
    middle = rest.astype(BF16).astype(F32)
    return high, middle, rest - middle


def terms_tile(top, total):
    rows, seqs = top.shape
    lane = lax.broadcasted_iota(jnp.int32, (rows, LANES), 1)
    tile = jnp.zeros((rows, LANES), F32)
    at = 0
    for part in three_terms(top) + three_terms(total):
        for b in range(seqs):
            tile = jnp.where(lane == at, part[:, b : b + 1], tile)
            at += 1
    return tile.astype(BF16)


def from_terms(tile, seqs):
    tile = tile.astype(F32)
    part = [tile[:, k * seqs : (k + 1) * seqs] for k in range(6)]
    return part[0] + part[1] + part[2], part[3] + part[4] + part[5]


def rescaled(tiles, seqs):
    pairs = [from_terms(tile, seqs) for tile in tiles]
    top = functools.reduce(jnp.maximum, [t for t, _ in pairs])
    factors = [jnp.exp(t - top) for t, _ in pairs]
    total = sum(n * f for (_, n), f in zip(pairs, factors))
    return top, total, factors


def project_queries(copies, low_ref, weight_ref, out_ref, low, held, sems):
    pieces, _, width = held.shape
    first = pltpu.make_async_copy(low_ref, low, sems.at[pieces])
    first.start()
    loads = [
        pltpu.make_async_copy(
            weight_ref.at[:, pl.ds(k * width, width)], held.at[k], sems.at[k]
        )
        for k in range(pieces)
    ]
    for load in loads:
        load.start()
    first.wait()
    rows = low[...]
    per_chunk = pieces * copies // out_ref.shape[0]
    for k in range(pieces):
        loads[k].wait()
        part = jnp.dot(rows, held[k], preferred_element_type=F32).astype(out_ref.dtype)
        chunk, at = divmod(k, per_chunk)
        for n in range(copies):
            out_ref[chunk * copies + n, :, at * width : (at + 1) * width] = part


def sum_queries(parts_ref, _, out_ref, rows):
    peers, seqs, _ = parts_ref.shape
    width = out_ref.shape[2]
    heads = out_ref.shape[1] // seqs
    total = parts_ref[0].astype(F32)
    for k in range(1, peers):
        total = total + parts_ref[k].astype(F32)
    for b in range(seqs):
        for j in range(heads):
            rows[b * heads + j : b * heads + j + 1, :] = total[
                b : b + 1, j * width : (j + 1) * width
            ]
    done = rows[...].astype(BF16)
    for k in range(out_ref.shape[0]):
        out_ref[k] = done


def attend(lengths_ref, query_ref, own_ref, other_ref, *refs):
    *outs, rows, out_ref = refs
    groups, both, width = query_ref.shape
    seqs, _, span = own_ref.shape
    each = both // seqs
    heads = groups * each
    core = lax.axis_index("head_1")
    pair = (
        lax.axis_index(CTX) * lax.axis_size("head_0") + lax.axis_index("head_0")
    ) * lax.axis_size("head_1")
    starts = ((pair + core) * span, (pair + 1 - core) * span)
    for g in range(groups):
        for b in range(seqs):
            rows[b, g * each : (g + 1) * each, :] = query_ref[
                g, b * each : (b + 1) * each, :
            ].astype(F32)
    tops, totals = [], []
    place = lax.broadcasted_iota(jnp.int32, (heads, span), 1)
    share = out_ref.shape[1]
    for b in range(seqs):
        query = rows[b].astype(BF16)
        scores = []
        for start, block in zip(starts, (own_ref, other_ref)):
            raw = jnp.dot(query, block[b], preferred_element_type=F32)
            scores.append(jnp.where(place < lengths_ref[:, b : b + 1] - start, raw * SCALE, MASKED))
        top = jnp.maximum(
            jnp.max(scores[0], axis=1, keepdims=True),
            jnp.max(scores[1], axis=1, keepdims=True),
        )
        top = jnp.maximum(top, FLOOR)
        weights = [jnp.exp(s - top) for s in scores]
        total = jnp.sum(weights[0], axis=1, keepdims=True) + jnp.sum(
            weights[1], axis=1, keepdims=True
        )
        numerator = sum(
            lax.dot_general(
                block[b, :KV_RANK, :], w.astype(BF16), LAST, preferred_element_type=F32
            )
            for w, block in zip(weights, (own_ref, other_ref))
        )
        numerator = numerator.T.astype(BF16)
        for k in range(out_ref.shape[0]):
            out_ref[k, :, b * KV_RANK : (b + 1) * KV_RANK] = numerator[
                k * share : (k + 1) * share
            ]
        tops.append(top)
        totals.append(total)
    lane = lax.broadcasted_iota(jnp.int32, (heads, LANES), 1)
    top = jnp.where(lane == 0, tops[0], tops[1])[:, :seqs]
    total = jnp.where(lane == 0, totals[0], totals[1])[:, :seqs]
    tile = terms_tile(top, total)
    for k in range(out_ref.shape[0]):
        out_ref[k, :, seqs * KV_RANK :] = tile[k * share : (k + 1) * share]
    for k in range(len(outs)):
        outs[k][...] = out_ref[lax.rem(lax.axis_index("head_0") + k, len(outs))]


def project_values(*refs):
    *parts, weight_ref, out_ref = refs
    peers = len(parts)
    heads, width = parts[0].shape
    seqs = (width - LANES) // KV_RANK
    top, total, factors = rescaled([part[:, width - LANES :] for part in parts], seqs)
    halves = []
    for b in range(seqs):
        halves.append(
            sum(
                parts[k][:, b * KV_RANK : (b + 1) * KV_RANK].astype(F32)
                * factors[k][:, b : b + 1]
                for k in range(peers)
            )
        )
    stacked = jnp.concatenate(halves, axis=0).astype(BF16)
    row = lax.broadcasted_iota(jnp.int32, (seqs * heads, LANES), 0)
    values = jnp.zeros((seqs * heads, LANES), F32)
    for h in range(heads):
        one = jnp.dot(stacked, weight_ref[h], preferred_element_type=F32)
        values = jnp.where(lax.rem(row, heads) == h, one, values)
    values = values.astype(BF16)
    tile = terms_tile(top, total)
    for k in range(out_ref.shape[0]):
        out_ref[k, : seqs * heads, :] = values
        out_ref[k, seqs * heads :, :] = tile


def project_output(parts_ref, weight_ref, out_ref, flat):
    peers, rows, lanes = parts_ref.shape
    seqs = out_ref.shape[1]
    heads = rows // (seqs + 1)
    _, total, factors = rescaled(
        [parts_ref[k, seqs * heads :, :] for k in range(peers)], seqs
    )
    for b in range(seqs):
        values = sum(
            parts_ref[k, b * heads : (b + 1) * heads, :].astype(F32) * factors[k][:, b : b + 1]
            for k in range(peers)
        )
        values = values / total[:, b : b + 1]
        for h in range(heads):
            flat[b : b + 1, h * lanes : (h + 1) * lanes] = values[h : h + 1]
    result = lax.dot_general(
        flat[...].astype(BF16), weight_ref[...], LAST, preferred_element_type=F32
    )
    width = out_ref.shape[2]
    for k in range(out_ref.shape[0]):
        out_ref[k] = result[:, k * width : (k + 1) * width]


def call(body, name, out_shape, out_dtype, in_specs, scratch=(), limit=8, outs=None):
    shape = pltpu.VMEM(out_shape, out_dtype)
    return pl.pallas_call(
        body,
        name=name,
        out_shape=[shape] * outs if outs else shape,
        in_specs=in_specs,
        out_specs=[VMEM] * outs if outs else VMEM,
        scratch_shapes=list(scratch),
        compiler_params=pltpu.CompilerParams(vmem_limit_bytes=int(limit * 2**20)),
    )


def on_device(query_low, query_weight, latent_cache, lengths, value_weight, output_weight):
    ctx_count = lax.axis_size(CTX)
    head_count = lax.axis_size(HEAD)
    chunks = lax.axis_size("ctx_0")
    depth_count = lax.axis_size("head_0")
    seqs, depth = query_low.shape
    local_heads = value_weight.shape[0]
    width = latent_cache.shape[2]
    columns = query_weight.shape[1]
    each = local_heads // chunks

    pieces = 2 * chunks
    partial = call(
        functools.partial(project_queries, ctx_count // chunks),
        "project_queries",
        (ctx_count, seqs, columns // chunks),
        BF16,
        [HBM, HBM],
        [
            pltpu.VMEM((seqs, depth), BF16),
            pltpu.VMEM((pieces, depth, columns // pieces), BF16),
            pltpu.SemaphoreType.DMA((pieces + 1,)),
        ],
        limit=62,
    )(query_low, query_weight)
    partial, latent_cache = lax.optimization_barrier((partial, latent_cache))
    latent_cache = jnp.swapaxes(latent_cache, 1, 2)
    other_cache = lax.ppermute(latent_cache, "head_1", [(0, 1), (1, 0)])
    partial = exchange(partial, CTX)

    own = call(
        sum_queries,
        "sum_queries",
        (depth_count * chunks, seqs * each, width),
        BF16,
        [VMEM, HBM],
        [pltpu.VMEM((seqs * each, width), F32)],
        limit=52.5,
    )(partial, latent_cache)
    queries = exchange(own, GATHER)

    packed = seqs * KV_RANK + LANES
    sent = call(
        attend,
        "attend",
        (local_heads, packed),
        BF16,
        [VMEM, VMEM, VMEM, VMEM],
        [
            pltpu.VMEM((seqs, depth_count * local_heads, width), F32),
            pltpu.VMEM((depth_count, local_heads, packed), BF16),
        ],
        limit=24,
        outs=depth_count,
    )(lengths.reshape(1, -1), queries, latent_cache, other_cache)
    arrived = [sent[0]] + [
        lax.ppermute(
            sent[k], "head_0", [(z, (z + k) % depth_count) for z in range(depth_count)]
        )
        for k in (2, 3, 1)
    ]

    values = call(
        project_values,
        "project_values",
        (ctx_count, (seqs + 1) * local_heads, value_weight.shape[2]),
        BF16,
        [VMEM] * (depth_count + 1),
    )(*arrived, value_weight)
    values = exchange(values, CTX)

    projected = call(
        project_output,
        "project_output",
        (head_count, seqs, output_weight.shape[1] // head_count),
        F32,
        [VMEM, VMEM],
        [pltpu.VMEM((seqs, output_weight.shape[0]), F32)],
    )(values, output_weight.T)
    return exchange(projected, HEAD).sum(axis=0).astype(BF16)


def solution(mesh):
    finer = Mesh(mesh.devices.reshape(4, 4, 4, 2), CTX_HEAD)
    return jax.shard_map(
        on_device,
        mesh=finer,
        in_specs=(
            P(None, CTX),
            P(CTX, HEAD),
            P(None, CTX_HEAD, None),
            P(),
            P(HEAD, None, None),
            P(HEAD, CTX),
        ),
        out_specs=P(None, CTX_HEAD),
        check_vma=False,
    )
```

```python
import functools

import jax
import jax.numpy as jnp
from jax import lax
from jax.experimental import pallas as pl
from jax.experimental.pallas import tpu as pltpu
from jax.sharding import Mesh
from jax.sharding import PartitionSpec as P

KV_RANK = 512
CTX = ("ctx_0", "ctx_1")
HEAD = ("head_0", "head_1")
CTX_HEAD = CTX + HEAD
GATHER = ("head_0", "ctx_0")
SCALE = 0.07216878
MASKED = -1e30
FLOOR = -1e29
LANES = 128
LAST = (((1,), (1,)), ((), ()))
F32 = jnp.float32
BF16 = jnp.bfloat16

VMEM = pl.BlockSpec(memory_space=pltpu.VMEM)
HBM = pl.BlockSpec(memory_space=pltpu.HBM)


def exchange(x, axes):
    return lax.all_to_all(x, axes, 0, 0, tiled=True)


def three_terms(x):
    high = x.astype(BF16).astype(F32)
    rest = x - high
    middle = rest.astype(BF16).astype(F32)
    return high, middle, rest - middle


def terms_tile(tops, totals):
    rows = tops[0].shape[0]
    lane = lax.broadcasted_iota(jnp.int32, (rows, LANES), 1)
    tile = jnp.zeros((rows, LANES), F32)
    at = 0
    for values in (tops, totals):
        for term in zip(*[three_terms(v) for v in values]):
            for part in term:
                tile = jnp.where(lane == at, part, tile)
                at += 1
    return tile.astype(BF16)


def spread(tiles, seqs):
    row = lax.broadcasted_iota(jnp.int32, (LANES, LANES), 0)
    picks = []
    for first in [3 * seqs * kind + b for kind in range(2) for b in range(seqs)]:
        hit = (row == first) | (row == first + seqs) | (row == first + 2 * seqs)
        picks.append(jnp.where(hit, 1.0, 0.0))
    pick = jnp.concatenate(picks, axis=1).astype(BF16)
    stacked = jnp.concatenate(tiles, axis=0)
    wide = jnp.dot(stacked, pick, preferred_element_type=F32)
    rows = tiles[0].shape[0]
    return [
        [
            wide[k * rows : (k + 1) * rows, n * LANES : (n + 1) * LANES]
            for n in range(2 * seqs)
        ]
        for k in range(len(tiles))
    ]


def rescaled(tiles, seqs):
    sums = spread(tiles, seqs)
    tops, totals, factors = [], [], []
    for b in range(seqs):
        top = functools.reduce(jnp.maximum, [part[b] for part in sums])
        factor = [jnp.exp(part[b] - top) for part in sums]
        tops.append(top)
        factors.append(factor)
        totals.append(sum(part[seqs + b] * f for part, f in zip(sums, factor)))
    return tops, totals, factors


def project_queries(copies, low_ref, weight_ref, out_ref, low, held, sems):
    pieces, _, width = held.shape
    first = pltpu.make_async_copy(low_ref, low, sems.at[pieces])
    first.start()
    loads = [
        pltpu.make_async_copy(
            weight_ref.at[:, pl.ds(k * width, width)], held.at[k], sems.at[k]
        )
        for k in range(pieces)
    ]
    for load in loads:
        load.start()
    first.wait()
    rows = low[...]
    per_chunk = pieces * copies // out_ref.shape[0]
    for k in range(pieces):
        loads[k].wait()
        part = jnp.dot(rows, held[k], preferred_element_type=F32).astype(out_ref.dtype)
        chunk, at = divmod(k, per_chunk)
        for n in range(copies):
            out_ref[chunk * copies + n, :, at * width : (at + 1) * width] = part


def sum_queries(parts_ref, _, out_ref, rows):
    peers, seqs, _ = parts_ref.shape
    width = out_ref.shape[2]
    heads = out_ref.shape[1] // seqs
    total = parts_ref[0].astype(F32)
    for k in range(1, peers):
        total = total + parts_ref[k].astype(F32)
    for b in range(seqs):
        for j in range(heads):
            rows[b * heads + j : b * heads + j + 1, :] = total[
                b : b + 1, j * width : (j + 1) * width
            ]
    done = rows[...].astype(BF16)
    for k in range(out_ref.shape[0]):
        out_ref[k] = done


def attend(lengths_ref, query_ref, own_ref, other_ref, *refs):
    *outs, rows, out_ref = refs
    groups, both, width = query_ref.shape
    seqs, _, span = own_ref.shape
    each = both // seqs
    heads = groups * each
    core = lax.axis_index("head_1")
    pair = (
        lax.axis_index(CTX) * lax.axis_size("head_0") + lax.axis_index("head_0")
    ) * lax.axis_size("head_1")
    starts = ((pair + core) * span, (pair + 1 - core) * span)
    for g in range(groups):
        for b in range(seqs):
            rows[b, g * each : (g + 1) * each, :] = query_ref[
                g, b * each : (b + 1) * each, :
            ].astype(F32)
    tops, totals = [], []
    place = lax.broadcasted_iota(jnp.int32, (heads, span), 1)
    share = out_ref.shape[1]
    for b in range(seqs):
        query = rows[b].astype(BF16)
        scores = []
        for start, block in zip(starts, (own_ref, other_ref)):
            raw = jnp.dot(query, block[b], preferred_element_type=F32)
            scores.append(jnp.where(place < lengths_ref[:, b : b + 1] - start, raw * SCALE, MASKED))
        top = jnp.maximum(
            jnp.max(scores[0], axis=1, keepdims=True),
            jnp.max(scores[1], axis=1, keepdims=True),
        )
        top = jnp.maximum(top, FLOOR)
        weights = [jnp.exp(s - top) for s in scores]
        total = jnp.sum(weights[0], axis=1, keepdims=True) + jnp.sum(
            weights[1], axis=1, keepdims=True
        )
        numerator = sum(
            lax.dot_general(
                block[b, :KV_RANK, :], w.astype(BF16), LAST, preferred_element_type=F32
            )
            for w, block in zip(weights, (own_ref, other_ref))
        )
        numerator = numerator.T.astype(BF16)
        for k in range(out_ref.shape[0]):
            out_ref[k, :, b * KV_RANK : (b + 1) * KV_RANK] = numerator[
                k * share : (k + 1) * share
            ]
        tops.append(top)
        totals.append(total)
    tile = terms_tile(tops, totals)
    for k in range(out_ref.shape[0]):
        out_ref[k, :, seqs * KV_RANK :] = tile[k * share : (k + 1) * share]
    for k in range(len(outs)):
        outs[k][...] = out_ref[lax.rem(lax.axis_index("head_0") + k, len(outs))]


def project_values(*refs):
    *parts, weight_ref, out_ref = refs
    peers = len(parts)
    heads, width = parts[0].shape
    seqs = (width - LANES) // KV_RANK
    tops, totals, factors = rescaled([part[:, width - LANES :] for part in parts], seqs)
    halves = []
    for b in range(seqs):
        halves.append(
            sum(
                parts[k][:, b * KV_RANK : (b + 1) * KV_RANK].astype(F32)
                * jnp.concatenate([factors[b][k]] * (KV_RANK // LANES), axis=1)
                for k in range(peers)
            )
        )
    stacked = jnp.concatenate(halves, axis=0).astype(BF16)
    row = lax.broadcasted_iota(jnp.int32, (seqs * heads, LANES), 0)
    values = jnp.zeros((seqs * heads, LANES), F32)
    for h in range(heads):
        one = jnp.dot(stacked, weight_ref[h], preferred_element_type=F32)
        values = jnp.where(lax.rem(row, heads) == h, one, values)
    values = values.astype(BF16)
    tile = terms_tile(tops, totals)
    for k in range(out_ref.shape[0]):
        out_ref[k, : seqs * heads, :] = values
        out_ref[k, seqs * heads :, :] = tile


def project_output(parts_ref, weight_ref, out_ref, flat):
    peers, rows, lanes = parts_ref.shape
    seqs = out_ref.shape[1]
    heads = rows // (seqs + 1)
    _, totals, factors = rescaled(
        [parts_ref[k, seqs * heads :, :] for k in range(peers)], seqs
    )
    for b in range(seqs):
        values = sum(
            parts_ref[k, b * heads : (b + 1) * heads, :].astype(F32) * factors[b][k]
            for k in range(peers)
        )
        values = values / totals[b]
        for h in range(heads):
            flat[b : b + 1, h * lanes : (h + 1) * lanes] = values[h : h + 1]
    result = lax.dot_general(
        flat[...].astype(BF16), weight_ref[...], LAST, preferred_element_type=F32
    )
    width = out_ref.shape[2]
    for k in range(out_ref.shape[0]):
        out_ref[k] = result[:, k * width : (k + 1) * width]


def call(body, name, out_shape, out_dtype, in_specs, scratch=(), limit=8, outs=None):
    shape = pltpu.VMEM(out_shape, out_dtype)
    return pl.pallas_call(
        body,
        name=name,
        out_shape=[shape] * outs if outs else shape,
        in_specs=in_specs,
        out_specs=[VMEM] * outs if outs else VMEM,
        scratch_shapes=list(scratch),
        compiler_params=pltpu.CompilerParams(vmem_limit_bytes=int(limit * 2**20)),
    )


def on_device(query_low, query_weight, latent_cache, lengths, value_weight, output_weight):
    ctx_count = lax.axis_size(CTX)
    head_count = lax.axis_size(HEAD)
    chunks = lax.axis_size("ctx_0")
    depth_count = lax.axis_size("head_0")
    seqs, depth = query_low.shape
    local_heads = value_weight.shape[0]
    width = latent_cache.shape[2]
    columns = query_weight.shape[1]
    each = local_heads // chunks

    pieces = chunks
    partial = call(
        functools.partial(project_queries, ctx_count // chunks),
        "project_queries",
        (ctx_count, seqs, columns // chunks),
        BF16,
        [HBM, HBM],
        [
            pltpu.VMEM((seqs, depth), BF16),
            pltpu.VMEM((pieces, depth, columns // pieces), BF16),
            pltpu.SemaphoreType.DMA((pieces + 1,)),
        ],
        limit=62,
    )(query_low, query_weight)
    partial, latent_cache = lax.optimization_barrier((partial, latent_cache))
    latent_cache = jnp.swapaxes(latent_cache, 1, 2)
    other_cache = lax.ppermute(latent_cache, "head_1", [(0, 1), (1, 0)])
    partial = exchange(partial, CTX)

    own = call(
        sum_queries,
        "sum_queries",
        (depth_count * chunks, seqs * each, width),
        BF16,
        [VMEM, HBM],
        [pltpu.VMEM((seqs * each, width), F32)],
        limit=52.5,
    )(partial, latent_cache)
    queries = exchange(own, GATHER)

    packed = seqs * KV_RANK + LANES
    sent = call(
        attend,
        "attend",
        (local_heads, packed),
        BF16,
        [VMEM, VMEM, VMEM, VMEM],
        [
            pltpu.VMEM((seqs, depth_count * local_heads, width), F32),
            pltpu.VMEM((depth_count, local_heads, packed), BF16),
        ],
        limit=24,
        outs=depth_count,
    )(lengths.reshape(1, -1), queries, latent_cache, other_cache)
    arrived = [sent[0]] + [
        lax.ppermute(
            sent[k], "head_0", [(z, (z + k) % depth_count) for z in range(depth_count)]
        )
        for k in (2, 3, 1)
    ]

    values = call(
        project_values,
        "project_values",
        (ctx_count, (seqs + 1) * local_heads, value_weight.shape[2]),
        BF16,
        [VMEM] * (depth_count + 1),
    )(*arrived, value_weight)
    values = exchange(values, CTX)

    projected = call(
        project_output,
        "project_output",
        (head_count, seqs, output_weight.shape[1] // head_count),
        F32,
        [VMEM, VMEM],
        [pltpu.VMEM((seqs, output_weight.shape[0]), F32)],
    )(values, output_weight.T)
    return exchange(projected, HEAD).sum(axis=0).astype(BF16)


def solution(mesh):
    finer = Mesh(mesh.devices.reshape(4, 4, 4, 2), CTX_HEAD)
    return jax.shard_map(
        on_device,
        mesh=finer,
        in_specs=(
            P(None, CTX),
            P(CTX, HEAD),
            P(None, CTX_HEAD, None),
            P(),
            P(HEAD, None, None),
            P(HEAD, CTX),
        ),
        out_specs=P(None, CTX_HEAD),
        check_vma=False,
    )
```

```python
import functools

import jax
import jax.numpy as jnp
from jax import lax
from jax.experimental import pallas as pl
from jax.experimental.pallas import tpu as pltpu
from jax.sharding import Mesh
from jax.sharding import PartitionSpec as P

KV_RANK = 512
CTX = ("ctx_0", "ctx_1")
HEAD = ("head_0", "head_1")
CTX_HEAD = CTX + HEAD
GATHER = ("head_0", "head_1", "ctx_0")
SCALE = 0.07216878
MASKED = -1e30
FLOOR = -1e29
LANES = 128
LAST = (((1,), (1,)), ((), ()))
F32 = jnp.float32
BF16 = jnp.bfloat16

VMEM = pl.BlockSpec(memory_space=pltpu.VMEM)
HBM = pl.BlockSpec(memory_space=pltpu.HBM)


def exchange(x, axes, groups=None):
    return lax.all_to_all(x, axes, 0, 0, tiled=True, axis_index_groups=groups)


def core_of(kind, z, depth):
    return kind ^ (2 * z // depth)


def along_depth(arrays, kinds):
    return [
        lax.ppermute(
            arrays[k],
            HEAD,
            [
                (2 * z + c, 2 * to[0] + to[1])
                for kind in kinds
                for (z, c), to in zip(kind, kind[k:] + kind[:k])
            ],
        )
        for k in reversed(range(1, len(arrays)))
    ]


def three_terms(x):
    high = x.astype(BF16).astype(F32)
    rest = x - high
    middle = rest.astype(BF16).astype(F32)
    return high, middle, rest - middle


def terms_tile(tops, totals):
    rows = tops[0].shape[0]
    lane = lax.broadcasted_iota(jnp.int32, (rows, LANES), 1)
    tile = jnp.zeros((rows, LANES), F32)
    at = 0
    for values in (tops, totals):
        for term in zip(*[three_terms(v) for v in values]):
            for part in term:
                tile = jnp.where(lane == at, part, tile)
                at += 1
    return tile.astype(BF16)


def spread(tiles, seqs):
    row = lax.broadcasted_iota(jnp.int32, (LANES, LANES), 0)
    picks = []
    for first in [3 * seqs * kind + b for kind in range(2) for b in range(seqs)]:
        hit = (row == first) | (row == first + seqs) | (row == first + 2 * seqs)
        picks.append(jnp.where(hit, 1.0, 0.0))
    pick = jnp.concatenate(picks, axis=1).astype(BF16)
    stacked = jnp.concatenate(tiles, axis=0)
    wide = jnp.dot(stacked, pick, preferred_element_type=F32)
    rows = tiles[0].shape[0]
    return [
        [
            wide[k * rows : (k + 1) * rows, n * LANES : (n + 1) * LANES]
            for n in range(2 * seqs)
        ]
        for k in range(len(tiles))
    ]


def rescaled(tiles, seqs):
    sums = spread(tiles, seqs)
    tops, totals, factors = [], [], []
    for b in range(seqs):
        top = functools.reduce(jnp.maximum, [part[b] for part in sums])
        factor = [jnp.exp(part[b] - top) for part in sums]
        tops.append(top)
        factors.append(factor)
        totals.append(sum(part[seqs + b] * f for part, f in zip(sums, factor)))
    return tops, totals, factors


def project_queries(copies, low_ref, weight_ref, out_ref, low, held, sems):
    pieces, _, width = held.shape
    first = pltpu.make_async_copy(low_ref, low, sems.at[pieces])
    first.start()
    loads = [
        pltpu.make_async_copy(
            weight_ref.at[:, pl.ds(k * width, width)], held.at[k], sems.at[k]
        )
        for k in range(pieces)
    ]
    for load in loads:
        load.start()
    first.wait()
    rows = low[...]
    per_chunk = pieces * copies // out_ref.shape[0]
    for k in range(pieces):
        loads[k].wait()
        part = jnp.dot(rows, held[k], preferred_element_type=F32).astype(out_ref.dtype)
        chunk, at = divmod(k, per_chunk)
        for n in range(copies):
            out_ref[chunk * copies + n, :, at * width : (at + 1) * width] = part


def sum_queries(parts_ref, _, out_ref, rows):
    peers, seqs, _ = parts_ref.shape
    width = out_ref.shape[2]
    heads = out_ref.shape[1] // seqs
    total = parts_ref[0].astype(F32)
    for k in range(1, peers):
        total = total + parts_ref[k].astype(F32)
    for b in range(seqs):
        for j in range(heads):
            rows[b * heads + j : b * heads + j + 1, :] = total[
                b : b + 1, j * width : (j + 1) * width
            ]
    done = rows[...].astype(BF16)
    for k in range(out_ref.shape[0]):
        out_ref[k] = done


def attend(lengths_ref, query_ref, own_ref, other_ref, *refs):
    *outs, rows, out_ref = refs
    groups, both, width = query_ref.shape
    seqs, _, span = own_ref.shape
    each = both // seqs
    heads = groups * each
    core = lax.axis_index("head_1")
    pair = (
        lax.axis_index(CTX) * lax.axis_size("head_0") + lax.axis_index("head_0")
    ) * lax.axis_size("head_1")
    starts = ((pair + core) * span, (pair + 1 - core) * span)
    for g in range(groups):
        for b in range(seqs):
            rows[b, g * each : (g + 1) * each, :] = query_ref[
                g, b * each : (b + 1) * each, :
            ].astype(F32)
    tops, totals = [], []
    place = lax.broadcasted_iota(jnp.int32, (heads, span), 1)
    share = out_ref.shape[1]
    for b in range(seqs):
        query = rows[b].astype(BF16)
        scores = []
        for start, block in zip(starts, (own_ref, other_ref)):
            raw = jnp.dot(query, block[b], preferred_element_type=F32)
            scores.append(jnp.where(place < lengths_ref[:, b : b + 1] - start, raw * SCALE, MASKED))
        top = jnp.maximum(
            jnp.max(scores[0], axis=1, keepdims=True),
            jnp.max(scores[1], axis=1, keepdims=True),
        )
        top = jnp.maximum(top, FLOOR)
        weights = [jnp.exp(s - top) for s in scores]
        total = jnp.sum(weights[0], axis=1, keepdims=True) + jnp.sum(
            weights[1], axis=1, keepdims=True
        )
        numerator = sum(
            lax.dot_general(
                block[b, :KV_RANK, :], w.astype(BF16), LAST, preferred_element_type=F32
            )
            for w, block in zip(weights, (own_ref, other_ref))
        )
        numerator = numerator.T.astype(BF16)
        for k in range(out_ref.shape[0]):
            out_ref[k, :, b * KV_RANK : (b + 1) * KV_RANK] = numerator[
                k * share : (k + 1) * share
            ]
        tops.append(top)
        totals.append(total)
    tile = terms_tile(tops, totals)
    for k in range(out_ref.shape[0]):
        out_ref[k, :, seqs * KV_RANK :] = tile[k * share : (k + 1) * share]
    for k in range(len(outs)):
        outs[k][...] = out_ref[lax.rem(lax.axis_index("head_0") + k, len(outs))]


def project_values(*refs):
    *parts, weight_ref, out_ref = refs
    peers = len(parts)
    heads, width = parts[0].shape
    seqs = (width - LANES) // KV_RANK
    tops, totals, factors = rescaled([part[:, width - LANES :] for part in parts], seqs)
    halves = []
    for b in range(seqs):
        halves.append(
            sum(
                parts[k][:, b * KV_RANK : (b + 1) * KV_RANK].astype(F32)
                * jnp.concatenate([factors[b][k]] * (KV_RANK // LANES), axis=1)
                for k in range(peers)
            )
        )
    stacked = jnp.concatenate(halves, axis=0).astype(BF16)
    row = lax.broadcasted_iota(jnp.int32, (seqs * heads, LANES), 0)
    values = jnp.zeros((seqs * heads, LANES), F32)
    for h in range(heads):
        one = jnp.dot(stacked, weight_ref[h], preferred_element_type=F32)
        values = jnp.where(lax.rem(row, heads) == h, one, values)
    values = values.astype(BF16)
    tile = terms_tile(tops, totals)
    for k in range(out_ref.shape[0]):
        out_ref[k, : seqs * heads, :] = values
        out_ref[k, seqs * heads :, :] = tile


def project_output(parts_ref, weight_ref, mine_ref, other_ref, flat, shares):
    peers, rows, lanes = parts_ref.shape
    seqs = shares.shape[1]
    heads = rows // (seqs + 1)
    _, totals, factors = rescaled(
        [parts_ref[k, seqs * heads :, :] for k in range(peers)], seqs
    )
    for b in range(seqs):
        values = sum(
            parts_ref[k, b * heads : (b + 1) * heads, :].astype(F32) * factors[b][k]
            for k in range(peers)
        )
        values = values / totals[b]
        for h in range(heads):
            flat[b : b + 1, h * lanes : (h + 1) * lanes] = values[h : h + 1]
    result = lax.dot_general(
        flat[...].astype(BF16), weight_ref[...], LAST, preferred_element_type=F32
    )
    width = shares.shape[2]
    for k in range(shares.shape[0]):
        shares[k] = result[:, k * width : (k + 1) * width]
    z, core = lax.axis_index("head_0"), lax.axis_index("head_1")
    depth = mine_ref.shape[0]
    for k in range(depth):
        to = lax.rem(z + k, depth)
        own = lax.rem(core + 2 * z // depth + 2 * to // depth, 2)
        mine_ref[k] = shares[2 * to + own]
        other_ref[k] = shares[2 * to + 1 - own]


def add_pairs(mine_ref, other_ref, *outs):
    for k, out in enumerate(outs):
        out[...] = mine_ref[k] + other_ref[k]


def call(body, name, out_shape, out_dtype, in_specs, scratch=(), limit=8, outs=None):
    shape = pltpu.VMEM(out_shape, out_dtype)
    return pl.pallas_call(
        body,
        name=name,
        out_shape=[shape] * outs if outs else shape,
        in_specs=in_specs,
        out_specs=[VMEM] * outs if outs else VMEM,
        scratch_shapes=list(scratch),
        compiler_params=pltpu.CompilerParams(vmem_limit_bytes=int(limit * 2**20)),
    )


def on_device(query_low, query_weight, latent_cache, lengths, value_weight, output_weight):
    ctx_count = lax.axis_size(CTX)
    head_count = lax.axis_size(HEAD)
    chunks = lax.axis_size("ctx_0")
    depth_count = lax.axis_size("head_0")
    seqs, depth = query_low.shape
    local_heads = value_weight.shape[0]
    width = latent_cache.shape[2]
    columns = query_weight.shape[1]
    each = local_heads // chunks

    pieces = chunks
    partial = call(
        functools.partial(project_queries, ctx_count // chunks),
        "project_queries",
        (ctx_count, seqs, columns // chunks),
        BF16,
        [HBM, HBM],
        [
            pltpu.VMEM((seqs, depth), BF16),
            pltpu.VMEM((pieces, depth, columns // pieces), BF16),
            pltpu.SemaphoreType.DMA((pieces + 1,)),
        ],
        limit=62,
    )(query_low, query_weight)
    partial, latent_cache = lax.optimization_barrier((partial, latent_cache))
    latent_cache = jnp.swapaxes(latent_cache, 1, 2)
    other_cache = lax.ppermute(latent_cache, "head_1", [(0, 1), (1, 0)])
    partial = exchange(partial, CTX)

    own = call(
        sum_queries,
        "sum_queries",
        (depth_count * chunks, seqs * each, width),
        BF16,
        [VMEM, HBM],
        [pltpu.VMEM((seqs * each, width), F32)],
        limit=52.5,
    )(partial, latent_cache)
    kinds = [
        [(z, core_of(kind, z, depth_count)) for z in range(depth_count)] for kind in range(2)
    ]
    queries = exchange(
        own,
        GATHER,
        [[(2 * z + c) * chunks + x for z, c in kind for x in range(chunks)] for kind in kinds],
    )

    packed = seqs * KV_RANK + LANES
    sent = call(
        attend,
        "attend",
        (local_heads, packed),
        BF16,
        [VMEM, VMEM, VMEM, VMEM],
        [
            pltpu.VMEM((seqs, depth_count * local_heads, width), F32),
            pltpu.VMEM((depth_count, local_heads, packed), BF16),
        ],
        limit=24,
        outs=depth_count,
    )(lengths.reshape(1, -1), queries, latent_cache, other_cache)
    arrived = [sent[0]] + along_depth(sent, kinds)

    values = call(
        project_values,
        "project_values",
        (ctx_count, (seqs + 1) * local_heads, value_weight.shape[2]),
        BF16,
        [VMEM] * (depth_count + 1),
    )(*arrived, value_weight)
    values = exchange(values, CTX)

    share = output_weight.shape[1] // head_count
    mine, other = call(
        project_output,
        "project_output",
        (depth_count, seqs, share),
        F32,
        [VMEM, VMEM],
        [
            pltpu.VMEM((seqs, output_weight.shape[0]), F32),
            pltpu.VMEM((head_count, seqs, share), F32),
        ],
        outs=2,
    )(values, output_weight.T)
    other = lax.ppermute(other, "head_1", [(0, 1), (1, 0)])
    pairs = call(
        add_pairs, "add_pairs", (seqs, share), F32, [VMEM, VMEM], outs=depth_count
    )(mine, other)
    return sum([pairs[0]] + along_depth(pairs, kinds)).astype(BF16)


def solution(mesh):
    finer = Mesh(mesh.devices.reshape(4, 4, 4, 2), CTX_HEAD)
    return jax.shard_map(
        on_device,
        mesh=finer,
        in_specs=(
            P(None, CTX),
            P(CTX, HEAD),
            P(None, CTX_HEAD, None),
            P(),
            P(HEAD, None, None),
            P(HEAD, CTX),
        ),
        out_specs=P(None, CTX_HEAD),
        check_vma=False,
    )
```

```python
import functools

import jax
import jax.numpy as jnp
from jax import lax
from jax.experimental import pallas as pl
from jax.experimental.pallas import tpu as pltpu
from jax.sharding import Mesh
from jax.sharding import PartitionSpec as P

KV_RANK = 512
CTX = ("ctx_0", "ctx_1")
HEAD = ("head_0", "head_1")
CTX_HEAD = CTX + HEAD
GATHER = ("head_0", "head_1", "ctx_0")
SCALE = 0.07216878
MASKED = -1e30
FLOOR = -1e29
LANES = 128
CHUNKS = 2
FOLDS = 2
LAST = (((1,), (1,)), ((), ()))
F32 = jnp.float32
BF16 = jnp.bfloat16

VMEM = pl.BlockSpec(memory_space=pltpu.VMEM)
HBM = pl.BlockSpec(memory_space=pltpu.HBM)


def exchange(x, axes, groups=None):
    return lax.all_to_all(x, axes, 0, 0, tiled=True, axis_index_groups=groups)


def core_of(kind, z, depth):
    return kind ^ (2 * z // depth)


def along_depth(arrays, kinds):
    return [
        lax.ppermute(
            arrays[k],
            HEAD,
            [
                (2 * z + c, 2 * to[0] + to[1])
                for kind in kinds
                for (z, c), to in zip(kind, [kind[n ^ k] for n in range(len(kind))])
            ],
        )
        for k in (2, 3, 1)
    ]


def three_terms(x):
    high = x.astype(BF16).astype(F32)
    rest = x - high
    middle = rest.astype(BF16).astype(F32)
    return high, middle, rest - middle


def terms_tile(tops, totals):
    rows = tops[0].shape[0]
    lane = lax.broadcasted_iota(jnp.int32, (rows, LANES), 1)
    tile = jnp.zeros((rows, LANES), F32)
    at = 0
    for values in (tops, totals):
        for term in zip(*[three_terms(v) for v in values]):
            for part in term:
                tile = jnp.where(lane == at, part, tile)
                at += 1
    return tile.astype(BF16)


def folded(tile, folds):
    rows = tile.shape[0] // folds
    parts = [tile[n * rows : (n + 1) * rows].astype(F32) for n in range(folds)]
    step = LANES // folds
    return sum(
        [parts[0]] + [pltpu.roll(parts[n], n * step, 1) for n in range(1, folds)]
    ).astype(BF16)


def spread(tiles, seqs, folds=1):
    row = lax.broadcasted_iota(jnp.int32, (LANES, LANES), 0)
    picks = []
    for first in [
        LANES // folds * n + 3 * seqs * kind + b
        for n in range(folds)
        for kind in range(2)
        for b in range(seqs)
    ]:
        hit = (row == first) | (row == first + seqs) | (row == first + 2 * seqs)
        picks.append(jnp.where(hit, 1.0, 0.0))
    pick = jnp.concatenate(picks, axis=1).astype(BF16)
    stacked = jnp.concatenate(tiles, axis=0)
    wide = jnp.dot(stacked, pick, preferred_element_type=F32)
    rows = tiles[0].shape[0]
    return [
        [
            jnp.concatenate(
                [
                    wide[k * rows : (k + 1) * rows, m * LANES : (m + 1) * LANES]
                    for m in range(n, len(picks), 2 * seqs)
                ],
                axis=0,
            )
            for n in range(2 * seqs)
        ]
        for k in range(len(tiles))
    ]


def rescaled(tiles, seqs, folds=1):
    sums = spread(tiles, seqs, folds)
    tops, totals, factors = [], [], []
    for b in range(seqs):
        top = functools.reduce(jnp.maximum, [part[b] for part in sums])
        factor = [jnp.exp(part[b] - top) for part in sums]
        tops.append(top)
        factors.append(factor)
        totals.append(sum(part[seqs + b] * f for part, f in zip(sums, factor)))
    return tops, totals, factors


def project_queries(rows_x, low_ref, weight_ref, out_ref, low, held, sems):
    pieces, _, width = held.shape
    first = pltpu.make_async_copy(low_ref, low, sems.at[pieces])
    first.start()
    loads = [
        pltpu.make_async_copy(
            weight_ref.at[:, pl.ds(k * width, width)], held.at[k], sems.at[k]
        )
        for k in range(pieces)
    ]
    for load in loads:
        load.start()
    first.wait()
    rows = low[...]
    per_chunk = out_ref.shape[2] // width
    rows_y = out_ref.shape[0] // rows_x
    for k in range(pieces):
        loads[k].wait()
        part = jnp.dot(rows, held[k], preferred_element_type=F32).astype(out_ref.dtype)
        chunk, at = divmod(k, per_chunk)
        for x in range(chunk, rows_x, pieces // per_chunk):
            for n in range(x * rows_y, (x + 1) * rows_y):
                out_ref[n, :, at * width : (at + 1) * width] = part


def sum_queries(parts_ref, _, out_ref, rows):
    peers, seqs, _ = parts_ref.shape
    width = out_ref.shape[2]
    heads = out_ref.shape[1] // seqs
    total = parts_ref[0].astype(F32)
    for k in range(1, peers):
        total = total + parts_ref[k].astype(F32)
    for b in range(seqs):
        for j in range(heads):
            rows[b * heads + j : b * heads + j + 1, :] = total[
                b : b + 1, j * width : (j + 1) * width
            ]
    done = rows[...].astype(BF16)
    for k in range(out_ref.shape[0]):
        out_ref[k] = done


def attend(lengths_ref, query_ref, own_ref, other_ref, *refs):
    *outs, rows, out_ref = refs
    groups, both, width = query_ref.shape
    seqs, _, span = own_ref.shape
    each = both // seqs
    heads = groups * each
    core = lax.axis_index("head_1")
    pair = (
        lax.axis_index(CTX) * lax.axis_size("head_0") + lax.axis_index("head_0")
    ) * lax.axis_size("head_1")
    starts = ((pair + core) * span, (pair + 1 - core) * span)
    for g in range(groups):
        for b in range(seqs):
            rows[b, g * each : (g + 1) * each, :] = query_ref[
                g, b * each : (b + 1) * each, :
            ].astype(F32)
    tops, totals = [], []
    place = lax.broadcasted_iota(jnp.int32, (heads, span), 1)
    share = out_ref.shape[1]
    for b in range(seqs):
        query = rows[b].astype(BF16)
        scores = []
        for start, block in zip(starts, (own_ref, other_ref)):
            raw = jnp.dot(query, block[b], preferred_element_type=F32)
            scores.append(jnp.where(place < lengths_ref[:, b : b + 1] - start, raw * SCALE, MASKED))
        top = jnp.maximum(
            jnp.max(scores[0], axis=1, keepdims=True),
            jnp.max(scores[1], axis=1, keepdims=True),
        )
        top = jnp.maximum(top, FLOOR)
        weights = [jnp.exp(s - top) for s in scores]
        total = jnp.sum(weights[0], axis=1, keepdims=True) + jnp.sum(
            weights[1], axis=1, keepdims=True
        )
        numerator = sum(
            lax.dot_general(
                block[b, :KV_RANK, :], w.astype(BF16), LAST, preferred_element_type=F32
            )
            for w, block in zip(weights, (own_ref, other_ref))
        )
        numerator = numerator.T.astype(BF16)
        for k in range(out_ref.shape[0]):
            out_ref[k, :, b * KV_RANK : (b + 1) * KV_RANK] = numerator[
                k * share : (k + 1) * share
            ]
        tops.append(top)
        totals.append(total)
    tile = terms_tile(tops, totals)
    for k in range(out_ref.shape[0]):
        out_ref[k, :, seqs * KV_RANK :] = tile[k * share : (k + 1) * share]
    for k in range(len(outs)):
        outs[k][...] = out_ref[lax.bitwise_xor(lax.axis_index("head_0"), k)]


def project_values(*refs):
    *parts, weight_ref, out_ref = refs
    peers = len(parts)
    heads, width = parts[0].shape
    seqs = (width - LANES) // KV_RANK
    tops, totals, factors = rescaled([part[:, width - LANES :] for part in parts], seqs)
    halves = []
    for b in range(seqs):
        halves.append(
            sum(
                parts[k][:, b * KV_RANK : (b + 1) * KV_RANK].astype(F32)
                * jnp.concatenate([factors[b][k]] * (KV_RANK // LANES), axis=1)
                for k in range(peers)
            )
        )
    stacked = jnp.concatenate(halves, axis=0).astype(BF16)
    row = lax.broadcasted_iota(jnp.int32, (seqs * heads, LANES), 0)
    values = jnp.zeros((seqs * heads, LANES), F32)
    for h in range(heads):
        one = jnp.dot(stacked, weight_ref[h], preferred_element_type=F32)
        values = jnp.where(lax.rem(row, heads) == h, one, values)
    values = values.astype(BF16)
    tile = folded(terms_tile(tops, totals), FOLDS)
    for k in range(out_ref.shape[0]):
        out_ref[k, : seqs * heads, :] = values
        out_ref[k, seqs * heads :, :] = tile


def project_output(parts_ref, weight_ref, mine_ref, other_ref, flat, shares):
    peers, rows, lanes = parts_ref.shape
    seqs = shares.shape[1]
    heads = rows * FOLDS // (seqs * FOLDS + 1)
    _, totals, factors = rescaled(
        [parts_ref[k, seqs * heads :, :] for k in range(peers)], seqs, FOLDS
    )
    for b in range(seqs):
        values = sum(
            parts_ref[k, b * heads : (b + 1) * heads, :].astype(F32) * factors[b][k]
            for k in range(peers)
        )
        values = values / totals[b]
        for h in range(heads):
            flat[b : b + 1, h * lanes : (h + 1) * lanes] = values[h : h + 1]
    result = lax.dot_general(
        flat[...].astype(BF16), weight_ref[...], LAST, preferred_element_type=F32
    )
    width = shares.shape[2]
    for k in range(shares.shape[0]):
        shares[k] = result[:, k * width : (k + 1) * width]
    z, core = lax.axis_index("head_0"), lax.axis_index("head_1")
    depth = mine_ref.shape[0]
    for k in range(depth):
        to = lax.bitwise_xor(z, k)
        own = lax.rem(core + 2 * z // depth + 2 * to // depth, 2)
        mine_ref[k] = shares[2 * to + own]
        other_ref[k] = shares[2 * to + 1 - own]


def add_pairs(mine_ref, other_ref, *outs):
    for k, out in enumerate(outs):
        out[...] = mine_ref[k] + other_ref[k]


def call(body, name, out_shape, out_dtype, in_specs, scratch=(), limit=8, outs=None):
    shape = pltpu.VMEM(out_shape, out_dtype)
    return pl.pallas_call(
        body,
        name=name,
        out_shape=[shape] * outs if outs else shape,
        in_specs=in_specs,
        out_specs=[VMEM] * outs if outs else VMEM,
        scratch_shapes=list(scratch),
        compiler_params=pltpu.CompilerParams(vmem_limit_bytes=int(limit * 2**20)),
    )


def on_device(query_low, query_weight, latent_cache, lengths, value_weight, output_weight):
    ctx_count = lax.axis_size(CTX)
    head_count = lax.axis_size(HEAD)
    rows_x = lax.axis_size("ctx_0")
    chunks = CHUNKS
    depth_count = lax.axis_size("head_0")
    seqs, depth = query_low.shape
    local_heads = value_weight.shape[0]
    width = latent_cache.shape[2]
    columns = query_weight.shape[1]
    each = local_heads // chunks

    pieces = 2
    partial = call(
        functools.partial(project_queries, rows_x),
        "project_queries",
        (ctx_count, seqs, columns // chunks),
        BF16,
        [HBM, HBM],
        [
            pltpu.VMEM((seqs, depth), BF16),
            pltpu.VMEM((pieces, depth, columns // pieces), BF16),
            pltpu.SemaphoreType.DMA((pieces + 1,)),
        ],
        limit=62,
    )(query_low, query_weight)
    partial, latent_cache = lax.optimization_barrier((partial, latent_cache))
    latent_cache = jnp.swapaxes(latent_cache, 1, 2)
    other_cache = lax.ppermute(latent_cache, "head_1", [(0, 1), (1, 0)])
    partial = exchange(partial, CTX)

    own = call(
        sum_queries,
        "sum_queries",
        (depth_count * chunks, seqs * each, width),
        BF16,
        [VMEM, HBM],
        [pltpu.VMEM((seqs * each, width), F32)],
        limit=52.5,
    )(partial, latent_cache)
    kinds = [
        [(z, core_of(kind, z, depth_count)) for z in range(depth_count)] for kind in range(2)
    ]
    queries = exchange(
        own,
        GATHER,
        [
            [(2 * z + c) * rows_x + x for z, c in kind for x in range(near, near + chunks)]
            for kind in kinds
            for near in range(0, rows_x, chunks)
        ],
    )

    packed = seqs * KV_RANK + LANES
    sent = call(
        attend,
        "attend",
        (local_heads, packed),
        BF16,
        [VMEM, VMEM, VMEM, VMEM],
        [
            pltpu.VMEM((seqs, depth_count * local_heads, width), F32),
            pltpu.VMEM((depth_count, local_heads, packed), BF16),
        ],
        limit=24,
        outs=depth_count,
    )(lengths.reshape(1, -1), queries, latent_cache, other_cache)
    arrived = [sent[0]] + along_depth(sent, kinds)

    values = call(
        project_values,
        "project_values",
        (ctx_count, seqs * local_heads + local_heads // FOLDS, value_weight.shape[2]),
        BF16,
        [VMEM] * (depth_count + 1),
    )(*arrived, value_weight)
    values = exchange(values, CTX)

    share = output_weight.shape[1] // head_count
    mine, other = call(
        project_output,
        "project_output",
        (depth_count, seqs, share),
        F32,
        [VMEM, VMEM],
        [
            pltpu.VMEM((seqs, output_weight.shape[0]), F32),
            pltpu.VMEM((head_count, seqs, share), F32),
        ],
        outs=2,
    )(values, output_weight.T)
    other = lax.ppermute(other, "head_1", [(0, 1), (1, 0)])
    pairs = call(
        add_pairs, "add_pairs", (seqs, share), F32, [VMEM, VMEM], outs=depth_count
    )(mine, other)
    return sum([pairs[0]] + along_depth(pairs, kinds)).astype(BF16)


def solution(mesh):
    finer = Mesh(mesh.devices.reshape(4, 4, 4, 2), CTX_HEAD)
    return jax.shard_map(
        on_device,
        mesh=finer,
        in_specs=(
            P(None, CTX),
            P(CTX, HEAD),
            P(None, CTX_HEAD, None),
            P(),
            P(HEAD, None, None),
            P(HEAD, CTX),
        ),
        out_specs=P(None, CTX_HEAD),
        check_vma=False,
    )
```

```python
import functools

import jax
import jax.numpy as jnp
from jax import lax
from jax.experimental import pallas as pl
from jax.experimental.pallas import tpu as pltpu
from jax.sharding import Mesh
from jax.sharding import PartitionSpec as P

KV_RANK = 512
CTX = ("ctx_0", "ctx_1")
HEAD = ("head_0", "head_1")
CTX_HEAD = CTX + HEAD
GATHER = ("head_0", "head_1", "ctx_0")
SCALE = 0.07216878
MASKED = -1e30
FLOOR = -1e29
LANES = 128
CHUNKS = 4
FOLDS = 2
LAST = (((1,), (1,)), ((), ()))
F32 = jnp.float32
BF16 = jnp.bfloat16

VMEM = pl.BlockSpec(memory_space=pltpu.VMEM)
HBM = pl.BlockSpec(memory_space=pltpu.HBM)


def exchange(x, axes, groups=None):
    return lax.all_to_all(x, axes, 0, 0, tiled=True, axis_index_groups=groups)


def core_of(kind, z, depth):
    return kind ^ (2 * z // depth)


def along_depth(arrays, partner):
    depth = len(arrays)
    return [
        lax.ppermute(
            arrays[k],
            HEAD,
            [
                (2 * z + c, 2 * (z ^ k) + partner(z, c, k))
                for z in range(depth)
                for c in range(2)
            ],
        )
        for k in (2, 3, 1)
    ]


def three_terms(x):
    high = x.astype(BF16).astype(F32)
    rest = x - high
    middle = rest.astype(BF16).astype(F32)
    return high, middle, rest - middle


def terms_tile(tops, totals):
    rows = tops[0].shape[0]
    lane = lax.broadcasted_iota(jnp.int32, (rows, LANES), 1)
    tile = jnp.zeros((rows, LANES), F32)
    at = 0
    for values in (tops, totals):
        for term in zip(*[three_terms(v) for v in values]):
            for part in term:
                tile = jnp.where(lane == at, part, tile)
                at += 1
    return tile.astype(BF16)


def folded(tile, folds):
    rows = tile.shape[0] // folds
    parts = [tile[n * rows : (n + 1) * rows].astype(F32) for n in range(folds)]
    step = LANES // folds
    return sum(
        [parts[0]] + [pltpu.roll(parts[n], n * step, 1) for n in range(1, folds)]
    ).astype(BF16)


def spread(tiles, seqs, folds=1):
    row = lax.broadcasted_iota(jnp.int32, (LANES, LANES), 0)
    picks = []
    for first in [
        LANES // folds * n + 3 * seqs * kind + b
        for n in range(folds)
        for kind in range(2)
        for b in range(seqs)
    ]:
        hit = (row == first) | (row == first + seqs) | (row == first + 2 * seqs)
        picks.append(jnp.where(hit, 1.0, 0.0))
    pick = jnp.concatenate(picks, axis=1).astype(BF16)
    stacked = jnp.concatenate(tiles, axis=0)
    wide = jnp.dot(stacked, pick, preferred_element_type=F32)
    rows = tiles[0].shape[0]
    return [
        [
            jnp.concatenate(
                [
                    wide[k * rows : (k + 1) * rows, m * LANES : (m + 1) * LANES]
                    for m in range(n, len(picks), 2 * seqs)
                ],
                axis=0,
            )
            for n in range(2 * seqs)
        ]
        for k in range(len(tiles))
    ]


def rescaled(tiles, seqs, folds=1):
    sums = spread(tiles, seqs, folds)
    tops, totals, factors = [], [], []
    for b in range(seqs):
        top = functools.reduce(jnp.maximum, [part[b] for part in sums])
        factor = [jnp.exp(part[b] - top) for part in sums]
        tops.append(top)
        factors.append(factor)
        totals.append(sum(part[seqs + b] * f for part, f in zip(sums, factor)))
    return tops, totals, factors


def project_queries(rows_x, low_ref, weight_ref, out_ref, low, held, sems):
    pieces, _, width = held.shape
    first = pltpu.make_async_copy(low_ref, low, sems.at[pieces])
    first.start()
    loads = [
        pltpu.make_async_copy(
            weight_ref.at[:, pl.ds(k * width, width)], held.at[k], sems.at[k]
        )
        for k in range(pieces)
    ]
    for load in loads:
        load.start()
    first.wait()
    rows = low[...]
    span = out_ref.shape[2]
    chunks = pieces * width // span
    rows_y = out_ref.shape[0] // rows_x
    for k in range(pieces):
        loads[k].wait()
        part = jnp.dot(rows, held[k], preferred_element_type=F32)
        for at in range(0, width, span):
            chunk = (k * width + at) // span
            for x in range(chunk, rows_x, chunks):
                for n in range(x * rows_y, (x + 1) * rows_y):
                    out_ref[n] = part[:, at : at + span]


def sum_queries(parts_ref, _, out_ref, rows):
    peers, seqs, _ = parts_ref.shape
    width = out_ref.shape[2]
    heads = out_ref.shape[1] // seqs
    total = parts_ref[0]
    for k in range(1, peers):
        total = total + parts_ref[k]
    for b in range(seqs):
        for j in range(heads):
            rows[b * heads + j : b * heads + j + 1, :] = total[
                b : b + 1, j * width : (j + 1) * width
            ]
    done = rows[...].astype(BF16)
    for k in range(out_ref.shape[0]):
        out_ref[k] = done


def attend(lengths_ref, query_ref, own_ref, other_ref, *refs):
    *outs, rows, out_ref = refs
    groups, both, width = query_ref.shape
    seqs, _, span = own_ref.shape
    each = both // seqs
    heads = groups * each
    core = lax.axis_index("head_1")
    pair = (
        lax.axis_index(CTX) * lax.axis_size("head_0") + lax.axis_index("head_0")
    ) * lax.axis_size("head_1")
    starts = ((pair + core) * span, (pair + 1 - core) * span)
    for g in range(groups):
        for b in range(seqs):
            rows[b, g * each : (g + 1) * each, :] = query_ref[
                g, b * each : (b + 1) * each, :
            ].astype(F32)
    tops, totals = [], []
    place = lax.broadcasted_iota(jnp.int32, (heads, span), 1)
    share = out_ref.shape[1]
    for b in range(seqs):
        query = rows[b].astype(BF16)
        scores = []
        for start, block in zip(starts, (own_ref, other_ref)):
            raw = jnp.dot(query, block[b], preferred_element_type=F32)
            scores.append(jnp.where(place < lengths_ref[:, b : b + 1] - start, raw * SCALE, MASKED))
        top = jnp.maximum(
            jnp.max(scores[0], axis=1, keepdims=True),
            jnp.max(scores[1], axis=1, keepdims=True),
        )
        top = jnp.maximum(top, FLOOR)
        weights = [jnp.exp(s - top) for s in scores]
        total = jnp.sum(weights[0], axis=1, keepdims=True) + jnp.sum(
            weights[1], axis=1, keepdims=True
        )
        numerator = sum(
            lax.dot_general(
                block[b, :KV_RANK, :], w.astype(BF16), LAST, preferred_element_type=F32
            )
            for w, block in zip(weights, (own_ref, other_ref))
        )
        numerator = numerator.T.astype(BF16)
        for k in range(out_ref.shape[0]):
            out_ref[k, :, b * KV_RANK : (b + 1) * KV_RANK] = numerator[
                k * share : (k + 1) * share
            ]
        tops.append(top)
        totals.append(total)
    tile = terms_tile(tops, totals)
    for k in range(out_ref.shape[0]):
        out_ref[k, :, seqs * KV_RANK :] = tile[k * share : (k + 1) * share]
    for k in range(len(outs)):
        outs[k][...] = out_ref[lax.bitwise_xor(lax.axis_index("head_0"), k)]


def project_values(*refs):
    *parts, weight_ref, out_ref = refs
    peers = len(parts)
    heads, width = parts[0].shape
    seqs = (width - LANES) // KV_RANK
    tops, totals, factors = rescaled([part[:, width - LANES :] for part in parts], seqs)
    halves = []
    for b in range(seqs):
        halves.append(
            sum(
                parts[k][:, b * KV_RANK : (b + 1) * KV_RANK].astype(F32)
                * jnp.concatenate([factors[b][k]] * (KV_RANK // LANES), axis=1)
                for k in range(peers)
            )
        )
    stacked = jnp.concatenate(halves, axis=0).astype(BF16)
    row = lax.broadcasted_iota(jnp.int32, (seqs * heads, LANES), 0)
    values = jnp.zeros((seqs * heads, LANES), F32)
    for h in range(heads):
        one = jnp.dot(stacked, weight_ref[h], preferred_element_type=F32)
        values = jnp.where(lax.rem(row, heads) == h, one, values)
    values = values.astype(BF16)
    tile = folded(terms_tile(tops, totals), FOLDS)
    for k in range(out_ref.shape[0]):
        out_ref[k, : seqs * heads, :] = values
        out_ref[k, seqs * heads :, :] = tile


def project_output(parts_ref, weight_ref, mine_ref, other_ref, flat, shares):
    peers, rows, lanes = parts_ref.shape
    seqs = shares.shape[1]
    heads = rows * FOLDS // (seqs * FOLDS + 1)
    _, totals, factors = rescaled(
        [parts_ref[k, seqs * heads :, :] for k in range(peers)], seqs, FOLDS
    )
    for b in range(seqs):
        values = sum(
            parts_ref[k, b * heads : (b + 1) * heads, :].astype(F32) * factors[b][k]
            for k in range(peers)
        )
        values = values / totals[b]
        for h in range(heads):
            flat[b : b + 1, h * lanes : (h + 1) * lanes] = values[h : h + 1]
    result = lax.dot_general(
        flat[...].astype(BF16), weight_ref[...], LAST, preferred_element_type=F32
    )
    width = shares.shape[2]
    for k in range(shares.shape[0]):
        shares[k] = result[:, k * width : (k + 1) * width]
    z, core = lax.axis_index("head_0"), lax.axis_index("head_1")
    for k in range(mine_ref.shape[0]):
        to = lax.bitwise_xor(z, k)
        own = core if k == 0 else 1 - core
        mine_ref[k] = shares[2 * to + own]
        other_ref[k] = shares[2 * to + 1 - own]


def add_pairs(mine_ref, other_ref, *outs):
    for k, out in enumerate(outs):
        out[...] = mine_ref[k] + other_ref[k]


def call(body, name, out_shape, out_dtype, in_specs, scratch=(), limit=8, outs=None):
    shape = pltpu.VMEM(out_shape, out_dtype)
    return pl.pallas_call(
        body,
        name=name,
        out_shape=[shape] * outs if outs else shape,
        in_specs=in_specs,
        out_specs=[VMEM] * outs if outs else VMEM,
        scratch_shapes=list(scratch),
        compiler_params=pltpu.CompilerParams(vmem_limit_bytes=int(limit * 2**20)),
    )


def on_device(query_low, query_weight, latent_cache, lengths, value_weight, output_weight):
    ctx_count = lax.axis_size(CTX)
    head_count = lax.axis_size(HEAD)
    rows_x = lax.axis_size("ctx_0")
    chunks = CHUNKS
    depth_count = lax.axis_size("head_0")
    seqs, depth = query_low.shape
    local_heads = value_weight.shape[0]
    width = latent_cache.shape[2]
    columns = query_weight.shape[1]
    each = local_heads // chunks

    pieces = 2
    partial = call(
        functools.partial(project_queries, rows_x),
        "project_queries",
        (ctx_count, seqs, columns // chunks),
        F32,
        [HBM, HBM],
        [
            pltpu.VMEM((seqs, depth), BF16),
            pltpu.VMEM((pieces, depth, columns // pieces), BF16),
            pltpu.SemaphoreType.DMA((pieces + 1,)),
        ],
        limit=62,
    )(query_low, query_weight)
    partial, latent_cache = lax.optimization_barrier((partial, latent_cache))
    latent_cache = jnp.swapaxes(latent_cache, 1, 2)
    other_cache = lax.ppermute(latent_cache, "head_1", [(0, 1), (1, 0)])
    partial = exchange(partial, CTX)

    own = call(
        sum_queries,
        "sum_queries",
        (depth_count * chunks, seqs * each, width),
        BF16,
        [VMEM, HBM],
        [pltpu.VMEM((seqs * each, width), F32)],
        limit=52.5,
    )(partial, latent_cache)
    kinds = [
        [(z, core_of(kind, z, depth_count)) for z in range(depth_count)] for kind in range(2)
    ]

    def same_kind(z, c, k):
        return core_of(core_of(c, z, depth_count), z ^ k, depth_count)

    queries = exchange(
        own,
        GATHER,
        [
            [(2 * z + c) * rows_x + x for z, c in kind for x in range(near, near + chunks)]
            for kind in kinds
            for near in range(0, rows_x, chunks)
        ],
    )

    packed = seqs * KV_RANK + LANES
    sent = call(
        attend,
        "attend",
        (local_heads, packed),
        BF16,
        [VMEM, VMEM, VMEM, VMEM],
        [
            pltpu.VMEM((seqs, depth_count * local_heads, width), F32),
            pltpu.VMEM((depth_count, local_heads, packed), BF16),
        ],
        limit=24,
        outs=depth_count,
    )(lengths.reshape(1, -1), queries, latent_cache, other_cache)
    arrived = [sent[0]] + along_depth(sent, same_kind)

    values = call(
        project_values,
        "project_values",
        (ctx_count, seqs * local_heads + local_heads // FOLDS, value_weight.shape[2]),
        BF16,
        [VMEM] * (depth_count + 1),
    )(*arrived, value_weight)
    values = exchange(values, CTX)

    share = output_weight.shape[1] // head_count
    mine, other = call(
        project_output,
        "project_output",
        (depth_count, seqs, share),
        F32,
        [VMEM, VMEM],
        [
            pltpu.VMEM((seqs, output_weight.shape[0]), F32),
            pltpu.VMEM((head_count, seqs, share), F32),
        ],
        outs=2,
    )(values, output_weight.T)
    other = lax.ppermute(other, "head_1", [(0, 1), (1, 0)])
    pairs = call(
        add_pairs, "add_pairs", (seqs, share), F32, [VMEM, VMEM], outs=depth_count
    )(mine, other)
    return sum([pairs[0]] + along_depth(pairs, lambda z, c, k: 1 - c)).astype(BF16)


def solution(mesh):
    finer = Mesh(mesh.devices.reshape(4, 4, 4, 2), CTX_HEAD)
    return jax.shard_map(
        on_device,
        mesh=finer,
        in_specs=(
            P(None, CTX),
            P(CTX, HEAD),
            P(None, CTX_HEAD, None),
            P(),
            P(HEAD, None, None),
            P(HEAD, CTX),
        ),
        out_specs=P(None, CTX_HEAD),
        check_vma=False,
    )
```

```python
import functools

import jax
import jax.numpy as jnp
from jax import lax
from jax.experimental import pallas as pl
from jax.experimental.pallas import tpu as pltpu
from jax.sharding import Mesh
from jax.sharding import PartitionSpec as P

KV_RANK = 512
CTX = ("ctx_0", "ctx_1")
HEAD = ("head_0", "head_1")
CTX_HEAD = CTX + HEAD
GATHER = ("head_0", "head_1", "ctx_0")
SCALE = 0.07216878
MASKED = -1e30
FLOOR = -1e29
LANES = 128
CHUNKS = 2
FOLDS = 2
LAST = (((1,), (1,)), ((), ()))
F32 = jnp.float32
BF16 = jnp.bfloat16
F16 = jnp.float16

VMEM = pl.BlockSpec(memory_space=pltpu.VMEM)
HBM = pl.BlockSpec(memory_space=pltpu.HBM)


def exchange(x, axes, groups=None):
    return lax.all_to_all(x, axes, 0, 0, tiled=True, axis_index_groups=groups)


def core_of(kind, z, depth):
    return kind ^ (2 * z // depth)


def along_depth(arrays, partner):
    depth = len(arrays)
    return [
        lax.ppermute(
            arrays[k],
            HEAD,
            [
                (2 * z + c, 2 * (z ^ k) + partner(z, c, k))
                for z in range(depth)
                for c in range(2)
            ],
        )
        for k in (2, 3, 1)
    ]


def three_terms(x):
    high = x.astype(BF16).astype(F32)
    rest = x - high
    middle = rest.astype(BF16).astype(F32)
    return high, middle, rest - middle


def terms_tile(tops, totals):
    rows = tops[0].shape[0]
    lane = lax.broadcasted_iota(jnp.int32, (rows, LANES), 1)
    tile = jnp.zeros((rows, LANES), F32)
    at = 0
    for values in (tops, totals):
        for term in zip(*[three_terms(v) for v in values]):
            for part in term:
                tile = jnp.where(lane == at, part, tile)
                at += 1
    return tile.astype(BF16)


def folded(tile, folds):
    rows = tile.shape[0] // folds
    parts = [tile[n * rows : (n + 1) * rows].astype(F32) for n in range(folds)]
    step = LANES // folds
    return sum(
        [parts[0]] + [pltpu.roll(parts[n], n * step, 1) for n in range(1, folds)]
    ).astype(BF16)


def spread(tiles, seqs, folds=1):
    row = lax.broadcasted_iota(jnp.int32, (LANES, LANES), 0)
    picks = []
    for first in [
        LANES // folds * n + 3 * seqs * kind + b
        for n in range(folds)
        for kind in range(2)
        for b in range(seqs)
    ]:
        hit = (row == first) | (row == first + seqs) | (row == first + 2 * seqs)
        picks.append(jnp.where(hit, 1.0, 0.0))
    pick = jnp.concatenate(picks, axis=1).astype(BF16)
    stacked = jnp.concatenate(tiles, axis=0)
    wide = jnp.dot(stacked, pick, preferred_element_type=F32)
    rows = tiles[0].shape[0]
    return [
        [
            jnp.concatenate(
                [
                    wide[k * rows : (k + 1) * rows, m * LANES : (m + 1) * LANES]
                    for m in range(n, len(picks), 2 * seqs)
                ],
                axis=0,
            )
            for n in range(2 * seqs)
        ]
        for k in range(len(tiles))
    ]


def rescaled(tiles, seqs, folds=1):
    sums = spread(tiles, seqs, folds)
    tops, totals, factors = [], [], []
    for b in range(seqs):
        top = functools.reduce(jnp.maximum, [part[b] for part in sums])
        factor = [jnp.exp(part[b] - top) for part in sums]
        tops.append(top)
        factors.append(factor)
        totals.append(sum(part[seqs + b] * f for part, f in zip(sums, factor)))
    return tops, totals, factors


def project_queries(low_ref, weight_ref, out_ref, low, held, sems):
    pieces, _, width = held.shape
    first = pltpu.make_async_copy(low_ref, low, sems.at[pieces])
    first.start()
    loads = [
        pltpu.make_async_copy(
            weight_ref.at[:, pl.ds(k * width, width)], held.at[k], sems.at[k]
        )
        for k in range(pieces)
    ]
    for load in loads:
        load.start()
    first.wait()
    rows = low[...]
    for k in range(pieces):
        loads[k].wait()
        out_ref[:, k * width : (k + 1) * width] = jnp.dot(
            rows, held[k], preferred_element_type=F32
        )


def sum_queries(parts_ref, _, out_ref, rows):
    total = parts_ref[...]
    seqs = total.shape[0]
    width = out_ref.shape[2]
    heads = out_ref.shape[1] // seqs
    for b in range(seqs):
        for j in range(heads):
            rows[b * heads + j : b * heads + j + 1, :] = total[
                b : b + 1, j * width : (j + 1) * width
            ]
    done = rows[...].astype(BF16)
    for k in range(out_ref.shape[0]):
        out_ref[k] = done


def attend(lengths_ref, query_ref, own_ref, other_ref, *refs):
    *outs, rows, out_ref = refs
    groups, both, width = query_ref.shape
    seqs, _, span = own_ref.shape
    each = both // seqs
    heads = groups * each
    core = lax.axis_index("head_1")
    pair = (
        lax.axis_index(CTX) * lax.axis_size("head_0") + lax.axis_index("head_0")
    ) * lax.axis_size("head_1")
    starts = ((pair + core) * span, (pair + 1 - core) * span)
    for g in range(groups):
        for b in range(seqs):
            rows[b, g * each : (g + 1) * each, :] = query_ref[
                g, b * each : (b + 1) * each, :
            ].astype(F32)
    tops, totals = [], []
    place = lax.broadcasted_iota(jnp.int32, (heads, span), 1)
    share = out_ref.shape[1]
    for b in range(seqs):
        query = rows[b].astype(BF16)
        scores = []
        for start, block in zip(starts, (own_ref, other_ref)):
            raw = jnp.dot(query, block[b], preferred_element_type=F32)
            scores.append(jnp.where(place < lengths_ref[:, b : b + 1] - start, raw * SCALE, MASKED))
        top = jnp.maximum(
            jnp.max(scores[0], axis=1, keepdims=True),
            jnp.max(scores[1], axis=1, keepdims=True),
        )
        top = jnp.maximum(top, FLOOR)
        weights = [jnp.exp(s - top) for s in scores]
        total = jnp.sum(weights[0], axis=1, keepdims=True) + jnp.sum(
            weights[1], axis=1, keepdims=True
        )
        numerator = sum(
            lax.dot_general(
                block[b, :KV_RANK, :], w.astype(BF16), LAST, preferred_element_type=F32
            )
            for w, block in zip(weights, (own_ref, other_ref))
        )
        numerator = numerator.T.astype(BF16)
        for k in range(out_ref.shape[0]):
            out_ref[k, :, b * KV_RANK : (b + 1) * KV_RANK] = numerator[
                k * share : (k + 1) * share
            ]
        tops.append(top)
        totals.append(total)
    tile = terms_tile(tops, totals)
    for k in range(out_ref.shape[0]):
        out_ref[k, :, seqs * KV_RANK :] = tile[k * share : (k + 1) * share]
    for k in range(len(outs)):
        outs[k][...] = out_ref[lax.bitwise_xor(lax.axis_index("head_0"), k)]


def project_values(*refs):
    *parts, weight_ref, out_ref = refs
    peers = len(parts)
    heads, width = parts[0].shape
    seqs = (width - LANES) // KV_RANK
    tops, totals, factors = rescaled([part[:, width - LANES :] for part in parts], seqs)
    halves = []
    for b in range(seqs):
        halves.append(
            sum(
                parts[k][:, b * KV_RANK : (b + 1) * KV_RANK].astype(F32)
                * jnp.concatenate([factors[b][k]] * (KV_RANK // LANES), axis=1)
                for k in range(peers)
            )
        )
    stacked = jnp.concatenate(halves, axis=0).astype(BF16)
    row = lax.broadcasted_iota(jnp.int32, (seqs * heads, LANES), 0)
    values = jnp.zeros((seqs * heads, LANES), F32)
    for h in range(heads):
        one = jnp.dot(stacked, weight_ref[h], preferred_element_type=F32)
        values = jnp.where(lax.rem(row, heads) == h, one, values)
    values = values.astype(BF16)
    tile = folded(terms_tile(tops, totals), FOLDS)
    for k in range(out_ref.shape[0]):
        out_ref[k, : seqs * heads, :] = values
        out_ref[k, seqs * heads :, :] = tile


def project_output(parts_ref, weight_ref, mine_ref, other_ref, flat, shares):
    peers, rows, lanes = parts_ref.shape
    seqs = shares.shape[1]
    heads = rows * FOLDS // (seqs * FOLDS + 1)
    _, totals, factors = rescaled(
        [parts_ref[k, seqs * heads :, :] for k in range(peers)], seqs, FOLDS
    )
    for b in range(seqs):
        values = sum(
            parts_ref[k, b * heads : (b + 1) * heads, :].astype(F32) * factors[b][k]
            for k in range(peers)
        )
        values = values / totals[b]
        for h in range(heads):
            flat[b : b + 1, h * lanes : (h + 1) * lanes] = values[h : h + 1]
    result = lax.dot_general(
        flat[...].astype(BF16), weight_ref[...], LAST, preferred_element_type=F32
    )
    width = shares.shape[2]
    for k in range(shares.shape[0]):
        shares[k] = result[:, k * width : (k + 1) * width]
    z, core = lax.axis_index("head_0"), lax.axis_index("head_1")
    for k in range(mine_ref.shape[0]):
        to = lax.bitwise_xor(z, k)
        own = core if k == 0 else 1 - core
        mine_ref[k] = shares[2 * to + own]
        other_ref[k] = shares[2 * to + 1 - own]


def add_pairs(mine_ref, other_ref, *outs):
    for k, out in enumerate(outs):
        out[...] = mine_ref[k] + other_ref[k]


def call(body, name, out_shape, out_dtype, in_specs, scratch=(), limit=8, outs=None):
    shape = pltpu.VMEM(out_shape, out_dtype)
    return pl.pallas_call(
        body,
        name=name,
        out_shape=[shape] * outs if outs else shape,
        in_specs=in_specs,
        out_specs=[VMEM] * outs if outs else VMEM,
        scratch_shapes=list(scratch),
        compiler_params=pltpu.CompilerParams(vmem_limit_bytes=int(limit * 2**20)),
    )


def on_device(query_low, query_weight, latent_cache, lengths, value_weight, output_weight):
    ctx_count = lax.axis_size(CTX)
    head_count = lax.axis_size(HEAD)
    rows_x = lax.axis_size("ctx_0")
    chunks = CHUNKS
    depth_count = lax.axis_size("head_0")
    seqs, depth = query_low.shape
    local_heads = value_weight.shape[0]
    width = latent_cache.shape[2]
    columns = query_weight.shape[1]
    each = local_heads // chunks

    pieces = 2
    partial = call(
        project_queries,
        "project_queries",
        (seqs, columns),
        F32,
        [HBM, HBM],
        [
            pltpu.VMEM((seqs, depth), BF16),
            pltpu.VMEM((pieces, depth, columns // pieces), BF16),
            pltpu.SemaphoreType.DMA((pieces + 1,)),
        ],
        limit=62,
    )(query_low, query_weight)
    partial, latent_cache = lax.optimization_barrier((partial, latent_cache))
    latent_cache = jnp.swapaxes(latent_cache, 1, 2)
    other_cache = lax.ppermute(latent_cache, "head_1", [(0, 1), (1, 0)])
    partial = jnp.swapaxes(partial.astype(F16).reshape(seqs, chunks, -1), 0, 1)
    partial = partial[None, :, None]
    partial = jnp.broadcast_to(
        partial, (rows_x // chunks, chunks, ctx_count // rows_x, *partial.shape[3:])
    )
    partial = exchange(partial.reshape(ctx_count, seqs, -1), CTX)
    partial = jnp.sum(partial.astype(F32), axis=0)

    own = call(
        sum_queries,
        "sum_queries",
        (depth_count * chunks, seqs * each, width),
        BF16,
        [VMEM, HBM],
        [pltpu.VMEM((seqs * each, width), F32)],
        limit=52.5,
    )(partial, latent_cache)
    kinds = [
        [(z, core_of(kind, z, depth_count)) for z in range(depth_count)] for kind in range(2)
    ]

    def same_kind(z, c, k):
        return core_of(core_of(c, z, depth_count), z ^ k, depth_count)

    queries = exchange(
        own,
        GATHER,
        [
            [(2 * z + c) * rows_x + x for z, c in kind for x in range(near, near + chunks)]
            for kind in kinds
            for near in range(0, rows_x, chunks)
        ],
    )

    packed = seqs * KV_RANK + LANES
    sent = call(
        attend,
        "attend",
        (local_heads, packed),
        BF16,
        [VMEM, VMEM, VMEM, VMEM],
        [
            pltpu.VMEM((seqs, depth_count * local_heads, width), F32),
            pltpu.VMEM((depth_count, local_heads, packed), BF16),
        ],
        limit=24,
        outs=depth_count,
    )(lengths.reshape(1, -1), queries, latent_cache, other_cache)
    arrived = [sent[0]] + along_depth(sent, same_kind)

    values = call(
        project_values,
        "project_values",
        (ctx_count, seqs * local_heads + local_heads // FOLDS, value_weight.shape[2]),
        BF16,
        [VMEM] * (depth_count + 1),
    )(*arrived, value_weight)
    values = exchange(values, CTX)

    share = output_weight.shape[1] // head_count
    mine, other = call(
        project_output,
        "project_output",
        (depth_count, seqs, share),
        F32,
        [VMEM, VMEM],
        [
            pltpu.VMEM((seqs, output_weight.shape[0]), F32),
            pltpu.VMEM((head_count, seqs, share), F32),
        ],
        outs=2,
    )(values, output_weight.T)
    other = lax.ppermute(other, "head_1", [(0, 1), (1, 0)])
    pairs = call(
        add_pairs, "add_pairs", (seqs, share), F32, [VMEM, VMEM], outs=depth_count
    )(mine, other)
    return sum([pairs[0]] + along_depth(pairs, lambda z, c, k: 1 - c)).astype(BF16)


def solution(mesh):
    finer = Mesh(mesh.devices.reshape(4, 4, 4, 2), CTX_HEAD)
    return jax.shard_map(
        on_device,
        mesh=finer,
        in_specs=(
            P(None, CTX),
            P(CTX, HEAD),
            P(None, CTX_HEAD, None),
            P(),
            P(HEAD, None, None),
            P(HEAD, CTX),
        ),
        out_specs=P(None, CTX_HEAD),
        check_vma=False,
    )
```
